32 devices in a mesh: role: 2 (over x), grp: 2 (over y), tp: 8 (over z, core).
Axes of the slice: x: 2, y: 2, z: 4, core: 2. Of those that a mesh axis runs over, the one named last changes fastest.
Arguments:
- queries: bfloat16 [2, 8, 8192], P(None, None, ('grp', 'tp')), may hold values from -130 to 130
- step_token_keys: bfloat16 [2, 8, 1024], replicated, may hold values from -6 to 6
- step_token_values: bfloat16 [2, 8, 1024], replicated, may hold values from -6 to 6
- stored_key_cache: bfloat16 [8, 512, 1024], P(None, ('grp', 'tp')), may hold values from -6 to 6
- stored_value_cache: bfloat16 [8, 512, 1024], P(None, ('grp', 'tp')), may hold values from -6 to 6
- lengths: int32 [8], replicated, may hold values from 2 to 512
- wo_sides: bfloat16 [2, 8192, 8192], P('role', ('grp', 'tp')), may hold values from -1 to 1
- gain_sides: float32 [2, 8192], P('role', ('grp', 'tp')), may hold values from 0.5 to 1.5
- head: bfloat16 [8192, 64128], P(None, ('grp', 'tp')), may hold values from -8 to 8
- resid: bfloat16 [2, 8, 8192], P(None, None, ('grp', 'tp')), may hold values from -90 to 90
- actions: int32 [2, 8], replicated, may hold values from 0 to 64127
Outputs:
- log_probs: float32 [2, 8], P('role')
- normed: bfloat16 [2, 8, 8192], P('role', None, ('grp', 'tp'))
The draws below stay inside these ranges and needn't reach their ends.
All inputs are finite; a program needn't handle non-finite values.
Results may differ from the reference program's by a relative error of at most 0.017.
Values may be sent and summed in bfloat16 or wider, within the bound.
A program may use at most 128 MiB of HBM per device.

```python
import math
import jax
import jax.numpy as jnp
from jax import lax

D = 8192
QUERY_HEADS = 64
KEY_VALUE_HEADS = 8
HEAD_SIZE = 128
V = 64128
DECODED_ROWS = 8
DECODE_STEPS = 2
HD = 8192
CACHE_SLOTS = 512


def key_table(key):
    return jnp.clip(jax.random.normal(jax.random.fold_in(key, 11), (DECODED_ROWS, CACHE_SLOTS, KEY_VALUE_HEADS * HEAD_SIZE), jnp.float32), -6.0, 6.0)


def draw_stored_key_cache(key, part):
    base_offset = key_table(key)
    return base_offset.astype(jnp.bfloat16)


def draw_queries(key, part):
    drawn = jnp.clip(jax.random.normal(jax.random.fold_in(key, 23), (DECODE_STEPS, DECODED_ROWS, QUERY_HEADS * HEAD_SIZE), jnp.float32), -6.0, 6.0)
    return drawn.astype(jnp.bfloat16)


def draw_resid(key, part):
    noise = jnp.clip(jax.random.normal(jax.random.fold_in(key, 31), (DECODE_STEPS, DECODED_ROWS, D), jnp.float32), -6.0, 6.0)
    ramp = 0.5 + jnp.arange(D, dtype=jnp.float32) / D
    values = noise * ramp[None, None, :]
    return values.astype(jnp.bfloat16)


def draw_head(key, part):
    base_offset = jnp.clip(jax.random.normal(jax.random.fold_in(key, 41), (D, V), jnp.float32), -6.0, 6.0) * (3.0 / math.sqrt(D))
    base_offset = jnp.clip(base_offset, -8.0, 8.0)
    return base_offset.astype(jnp.bfloat16)


def plant(array, stream_key, smallest, high):
    longest = array.shape.index(max(array.shape))
    spots = []
    for shift in (0, 1):
        where = [jax.random.randint(jax.random.fold_in(stream_key, axis), (), 0, length) for axis, length in enumerate(array.shape)]
        where[longest] = (where[longest] + shift) % array.shape[longest]
        spots.append(tuple(where))
    return array.at[spots[0]].set(smallest).at[spots[1]].set(high)


def block_levels(own_key, dims, cuts, smallest, high):
    def one(position, blocks):
        heights = jax.random.uniform(jax.random.fold_in(jax.random.fold_in(own_key, 6), position), (blocks,), jnp.float32, smallest / len(cuts), high / len(cuts))
        return jnp.repeat(jnp.exp(heights), dims[position] // blocks).reshape((-1,) + (1,) * (len(dims) - position - 1))

    level = one(*cuts[0])
    for cut in cuts[1:]:
        level = level * one(*cut)
    return level


def scatter_about(own_key, extent, spread, reach, cuts=(), kind=jnp.bfloat16):
    entries = spread * jax.random.normal(own_key, extent, jnp.float32)
    if cuts:
        entries = entries * block_levels(own_key, extent, cuts, -0.22, 0.18)
    return jnp.clip(entries, -reach, reach).astype(kind)


def setup_inputs(seed: int = 0) -> dict:
    splits = jax.random.split(jax.random.key(seed), 12)
    return {
        "queries": draw_queries(jax.random.fold_in(splits[11], 71), 0),
        "step_token_keys": scatter_about(splits[1], (DECODE_STEPS, DECODED_ROWS, KEY_VALUE_HEADS * HEAD_SIZE), 1.0, 6.0),
        "step_token_values": scatter_about(splits[2], (DECODE_STEPS, DECODED_ROWS, KEY_VALUE_HEADS * HEAD_SIZE), 1.0, 6.0),
        "stored_key_cache": draw_stored_key_cache(jax.random.fold_in(splits[11], 71), 0),
        "stored_value_cache": scatter_about(splits[4], (DECODED_ROWS, CACHE_SLOTS, KEY_VALUE_HEADS * HEAD_SIZE), 1.0, 6.0, ((1, 16),)),
        "lengths": plant(jax.random.randint(splits[5], (DECODED_ROWS,), 2, CACHE_SLOTS + 1), jax.random.fold_in(splits[5], 1), 2, CACHE_SLOTS).astype(jnp.int32),
        "wo_sides": scatter_about(splits[6], (2, HD, D), (max(HD // 256, 1)) ** -0.5, 1.0, ((0, 2), (1, 16))),
        "gain_sides": jnp.clip(1.0 + 0.1 * jax.random.normal(splits[7], (2, D), jnp.float32), 0.5, 1.5),
        "head": draw_head(jax.random.fold_in(splits[11], 71), 0),
        "resid": draw_resid(jax.random.fold_in(splits[11], 71), 0),
        "actions": plant(jax.random.randint(splits[10], (DECODE_STEPS, DECODED_ROWS), 0, V), jax.random.fold_in(splits[10], 1), 0, V - 1).astype(jnp.int32),
    }


def reference(queries, step_token_keys, step_token_values, stored_key_cache, stored_value_cache, lengths, wo_sides, gain_sides, head, resid, actions):
    count_of_rows = lengths.shape[0]
    query_group_width = QUERY_HEADS // KEY_VALUE_HEADS
    logit_scale = 1.0 / math.sqrt(HEAD_SIZE)
    positions = jnp.arange(CACHE_SLOTS, dtype=jnp.int32)
    valid = positions[None, :] < lengths[:, None]
    masking = valid[:, None, None, :]
    prior_keys = stored_key_cache.astype(jnp.float32).reshape(count_of_rows, CACHE_SLOTS, KEY_VALUE_HEADS, HEAD_SIZE)
    prior_values = stored_value_cache.astype(jnp.float32).reshape(count_of_rows, CACHE_SLOTS, KEY_VALUE_HEADS, HEAD_SIZE)
    vocab_ids = jnp.arange(V, dtype=jnp.int32)
    prob_list = []
    normed_list = []
    for decode_index in range(DECODE_STEPS):
        version = 1 - decode_index
        current_query = queries[decode_index].astype(jnp.float32).reshape(count_of_rows, KEY_VALUE_HEADS, query_group_width, HEAD_SIZE) * logit_scale
        scores = jnp.einsum('rkgd,rskd->rkgs', current_query, prior_keys)
        scores = jnp.where(masking, scores, -1e+30)
        incoming_keys = step_token_keys[:decode_index + 1].astype(jnp.float32).reshape(decode_index + 1, count_of_rows, KEY_VALUE_HEADS, HEAD_SIZE)
        incoming_values = step_token_values[:decode_index + 1].astype(jnp.float32).reshape(decode_index + 1, count_of_rows, KEY_VALUE_HEADS, HEAD_SIZE)
        fresh_scores = jnp.einsum('rkgd,trkd->rkgt', current_query, incoming_keys)
        highest = jnp.maximum(lax.optimization_barrier(jnp.max(scores, axis=-1)), lax.optimization_barrier(jnp.max(fresh_scores, axis=-1)))
        cache_probs = jnp.exp(scores - highest[..., None]) * masking
        fresh_probs = jnp.exp(fresh_scores - highest[..., None])
        totals = lax.optimization_barrier(jnp.sum(cache_probs, axis=-1)) + lax.optimization_barrier(jnp.sum(fresh_probs, axis=-1))
        weighted = jnp.einsum('rkgs,rskd->rkgd', cache_probs, prior_values) + jnp.einsum('rkgt,trkd->rkgd', fresh_probs, incoming_values)
        attended = (weighted / totals[..., None]).reshape(count_of_rows, QUERY_HEADS * HEAD_SIZE).astype(jnp.bfloat16)
        state = resid[decode_index].astype(jnp.float32) + jnp.dot(attended, wo_sides[version], preferred_element_type=jnp.float32)
        mean_square = lax.optimization_barrier(jnp.mean(state * state, axis=-1, keepdims=True))
        normed_now = (state * jax.lax.rsqrt(mean_square + 1e-05) * gain_sides[version][None, :]).astype(jnp.bfloat16)
        logits = jnp.dot(normed_now, head, preferred_element_type=jnp.float32)
        largest = lax.optimization_barrier(jnp.max(logits, axis=-1))
        exp_sum = lax.optimization_barrier(jnp.sum(jnp.exp(logits - largest[:, None]), axis=-1))
        is_target = vocab_ids[None, :] == actions[decode_index][:, None]
        target = lax.optimization_barrier(jnp.sum(jnp.where(is_target, logits, 0.0), axis=-1))
        prob_list.append(target - largest - jnp.log(exp_sum))
        normed_list.append(normed_now)
    return (jnp.stack(prob_list), jnp.stack(normed_list))
```

```python
import functools
import math

import jax
import jax.numpy as jnp
from jax import lax
from jax.experimental import pallas as pl
from jax.experimental.pallas import tpu as pltpu
from jax.sharding import PartitionSpec as P

D = 8192
QUERY_HEADS = 64
KEY_VALUE_HEADS = 8
HEAD_SIZE = 128
DECODE_STEPS = 2


def swap_sides(value):
    return lax.ppermute(value, "role", [(0, 1), (1, 0)])


def plain(
    queries,
    step_token_keys,
    step_token_values,
    stored_key_cache,
    stored_value_cache,
    lengths,
    wo_sides,
    gain_sides,
    head,
    resid,
    actions,
):
    both = ("grp", "tp")
    place = lax.axis_index(both)
    step = 1 - lax.axis_index("role")
    count_of_rows = lengths.shape[0]
    shard_length = stored_key_cache.shape[1]
    query_group_width = QUERY_HEADS // KEY_VALUE_HEADS
    logit_scale = 1.0 / math.sqrt(HEAD_SIZE)
    query_matrix = lax.all_gather(
        lax.dynamic_index_in_dim(queries, step, 0, keepdims=False), both, axis=1, tiled=True
    )
    positions = place * shard_length + jnp.arange(shard_length, dtype=jnp.int32)
    valid = positions[None, :] < lengths[:, None]
    masking = valid[:, None, None, :]
    cache_shape = (count_of_rows, shard_length, KEY_VALUE_HEADS, HEAD_SIZE)
    prior_keys = stored_key_cache.reshape(cache_shape)
    prior_values = stored_value_cache.reshape(cache_shape)
    step_shape = (DECODE_STEPS, count_of_rows, KEY_VALUE_HEADS, HEAD_SIZE)
    incoming_keys = step_token_keys.astype(jnp.float32).reshape(step_shape)
    incoming_values = step_token_values.astype(jnp.float32).reshape(step_shape)
    current_query = query_matrix.reshape(
        count_of_rows, KEY_VALUE_HEADS, query_group_width, HEAD_SIZE
    )
    scores = (
        jnp.einsum("rkgd,rskd->rkgs", current_query, prior_keys, preferred_element_type=jnp.float32)
        * logit_scale
    )
    scores = jnp.where(masking, scores, -1e30)
    fresh_live = jnp.arange(DECODE_STEPS, dtype=jnp.int32) <= step
    fresh_scores = (
        jnp.einsum("rkgd,trkd->rkgt", current_query.astype(jnp.float32), incoming_keys)
        * logit_scale
    )
    fresh_scores = jnp.where(fresh_live, fresh_scores, -1e30)
    fresh_highest = jnp.max(fresh_scores, axis=-1)
    overall = lax.pmax(jnp.maximum(jnp.max(scores, axis=-1), fresh_highest), both)
    cache_probs = jnp.exp(scores - overall[..., None]) * masking
    fresh_probs = jnp.exp(fresh_scores - overall[..., None]) * fresh_live
    fresh_probs = fresh_probs * (place == 0)
    totals = jnp.sum(cache_probs, axis=-1) + jnp.sum(fresh_probs, axis=-1)
    weighted = jnp.einsum(
        "rkgs,rskd->rkgd", cache_probs, prior_values.astype(jnp.float32)
    ) + jnp.einsum("rkgt,trkd->rkgd", fresh_probs, incoming_values)
    features = QUERY_HEADS * HEAD_SIZE
    mixed = lax.psum_scatter(
        weighted.reshape(count_of_rows, features), both, scatter_dimension=1, tiled=True
    )
    totals = lax.psum(totals.reshape(count_of_rows, QUERY_HEADS), both)
    feature_rows = wo_sides.shape[1]
    own_heads = (place * feature_rows + jnp.arange(feature_rows)) // HEAD_SIZE
    own_part = (mixed / jnp.take(totals, own_heads, axis=1)).astype(jnp.bfloat16)
    branch_out = lax.psum_scatter(
        jnp.dot(own_part, wo_sides[0], preferred_element_type=jnp.float32),
        both,
        scatter_dimension=1,
        tiled=True,
    )
    resid_now = lax.dynamic_index_in_dim(resid, step, 0, keepdims=False)
    state = resid_now.astype(jnp.float32) + branch_out
    square_sum = lax.psum(jnp.sum(state * state, axis=-1), both)
    normed_now = (
        state * lax.rsqrt(square_sum[:, None] / D + 1e-05) * gain_sides[0][None, :]
    ).astype(jnp.bfloat16)
    logits = jnp.dot(
        lax.all_gather(normed_now, both, axis=1, tiled=True),
        head,
        preferred_element_type=jnp.float32,
    )
    local_highest = jnp.max(logits, axis=-1)
    action_now = lax.dynamic_index_in_dim(actions, step, 0, keepdims=False)
    head_width = head.shape[1]
    vocab_ids = place * head_width + jnp.arange(head_width, dtype=jnp.int32)
    is_target = vocab_ids[None, :] == action_now[:, None]
    target = jnp.sum(jnp.where(is_target, logits, 0.0), axis=-1)
    exp_sum = jnp.sum(jnp.exp(logits - local_highest[:, None]), axis=-1)
    parts = lax.all_gather(jnp.stack([local_highest, exp_sum, target]), both)
    largest = jnp.max(parts[:, 0], axis=0)
    exp_sum = jnp.sum(parts[:, 1] * jnp.exp(parts[:, 0] - largest[None]), axis=0)
    prob_now = jnp.sum(parts[:, 2], axis=0) - largest - jnp.log(exp_sum)
    return (swap_sides(prob_now)[None], swap_sides(normed_now)[None])


LOW = -1e30
DEAD = -1e29
TILE = 256
MESH = pl.DeviceIdType.MESH


def fused_kernel(
    n,
    tp,
    queries,
    token_keys,
    token_values,
    keys_in,
    values_in,
    lengths_in,
    gain_in,
    resid_in,
    actions_in,
    wo,
    head,
    log_probs,
    normed,
    q_own,
    fresh_keys,
    fresh_values,
    lengths,
    actions,
    gain,
    resid,
    keys,
    values,
    wo_buf,
    head_buf,
    bias,
    q_all,
    b_send,
    b_recv,
    c_send,
    c_recv,
    x_all,
    s_send,
    s_recv,
    acc,
    n_send,
    n_recv,
    e_send,
    e_recv,
    in_sems,
    head_sems,
    q_ss,
    q_rs,
    k_ss,
    k_rs,
    b_ss,
    b_rs,
    c_ss,
    c_rs,
    d_ss,
    f_ss,
    x_rs,
    s_ss,
    s_rs,
    n_sems,
    e_ss,
    e_rs,
):
    role = lax.axis_index("role")
    me = lax.axis_index("grp") * tp + lax.axis_index("tp")
    core = me % 2
    chip = me // 2
    mate = me + 1 - 2 * core
    chips = n // 2
    near = chips // 2
    half = n // 2
    side = chip // near
    step = 1 - role
    rows = resid.shape[0]
    width = resid.shape[1]
    shard = keys.shape[2]
    half_keys = keys.shape[3]
    own_heads = width // HEAD_SIZE
    group = QUERY_HEADS // KEY_VALUE_HEADS
    slots = 2 * rows * shard
    vocab = head.shape[0]
    kept = head_buf.shape[0]
    tiles = acc.shape[0]
    scale = 1.0 / math.sqrt(HEAD_SIZE)
    f32 = jnp.float32
    bf16 = jnp.bfloat16

    def flip(index, by, size):
        out = index
        bit = 1
        while bit < size:
            if isinstance(by, int):
                if by // bit % 2:
                    out = out + bit - 2 * bit * (index // bit % 2)
            else:
                out = out + (by // bit % 2) * (bit - 2 * bit * (index // bit % 2))
            bit *= 2
        return out

    def remote(src, dst, ss, rs, to_role, place):
        return pltpu.make_async_remote_copy(
            src_ref=src,
            dst_ref=dst,
            send_sem=ss,
            recv_sem=rs,
            device_id=(to_role, place // tp, place % tp),
            device_id_type=MESH,
        )

    def landed(ref, sem):
        pltpu.make_async_copy(ref, ref, sem).wait()

    own_keys = pl.ds(pl.multiple_of(core * half_keys, 128), half_keys)
    mate_keys = pl.ds(pl.multiple_of((1 - core) * half_keys, 128), half_keys)
    chip_lanes = pl.ds(pl.multiple_of(chip * HEAD_SIZE, HEAD_SIZE), HEAD_SIZE)
    loads = [
        pltpu.make_async_copy(src, dst, in_sems.at[i])
        for i, (src, dst) in enumerate(
            [
                (queries.at[step], q_own),
                (lengths_in, lengths),
                (keys_in.at[:, :, own_keys], keys.at[core]),
                (values_in.at[:, :, own_keys], values.at[core]),
                (token_keys.at[:, :, chip_lanes], fresh_keys),
                (token_values.at[:, :, chip_lanes], fresh_values),
                (resid_in.at[step], resid),
                (gain_in, gain),
                (actions_in, actions),
                (wo.at[0], wo_buf),
            ]
        )
    ]
    for copy in loads:
        copy.start()
    first_row = pl.multiple_of(role * (vocab - kept), 8)

    def head_copy(p):
        lanes = pl.ds(pl.multiple_of(p * width, 128), width)
        return pltpu.make_async_copy(
            head.at[pl.ds(first_row, kept), lanes], head_buf.at[:, lanes], head_sems.at[p]
        )

    @pl.loop(0, n)
    def _(p):
        head_copy(p).start()

    barrier = pltpu.get_barrier_semaphore()
    for i in range(1, 2 * n):
        other = (role * n + me + i) % (2 * n)
        pl.semaphore_signal(
            barrier,
            inc=1,
            device_id=(other // n, other % n // tp, other % tp),
            device_id_type=MESH,
        )
    loads[0].wait()
    pl.semaphore_wait(barrier, 2 * n - 1)

    own_slot = me % half
    for i in range(chips - 1, 0, -1):
        to = 2 * flip(chip, i, chips) + side
        remote(q_own, q_all.at[own_slot], q_ss.at[i], q_rs.at[own_slot], role, to).start()

    @pl.when(core != side)
    def _():
        remote(q_own, q_all.at[own_slot], q_ss.at[0], q_rs.at[own_slot], role, mate).start()

    @pl.when(core == side)
    def _():
        q_all[own_slot] = q_own[...]

    key_swap = remote(
        keys_in.at[:, :, mate_keys], keys.at[core], k_ss.at[0], k_rs.at[0], role, mate
    )
    value_swap = remote(
        values_in.at[:, :, mate_keys], values.at[core], k_ss.at[1], k_rs.at[1], role, mate
    )
    key_swap.start()
    value_swap.start()

    loads[1].wait()
    row_ids = lax.broadcasted_iota(jnp.int32, (rows, slots), 0)
    col_ids = lax.broadcasted_iota(jnp.int32, (rows, slots), 1)
    limit = jnp.zeros((rows, slots), jnp.int32)
    for b in range(rows):
        limit = jnp.where(row_ids == b, lengths[b], limit)
    origin = col_ids // (rows * shard)
    place_ids = (2 * chip + origin) * shard + col_ids % shard
    live = (col_ids // shard % rows == row_ids) & (place_ids < limit)
    bias[...] = jnp.where(live, 0.0, LOW)

    loads[2].wait()
    loads[3].wait()
    ones = jnp.ones((slots, HEAD_SIZE), bf16)
    lane = lax.broadcasted_iota(jnp.int32, (rows, HEAD_SIZE), 1)

    def wait_query(slot):
        remote(q_own, q_all.at[slot], q_ss.at[0], q_rs.at[slot], role, me).wait_recv()

    for i in range(near):
        local = flip(chip % near, i, near)
        slot = 2 * local
        if i == 0:

            @pl.when(core == side)
            def _():
                wait_query(mate % half)

            @pl.when(core != side)
            def _():
                wait_query(slot)
                wait_query(slot + 1)

            remote(
                keys_in.at[:, :, mate_keys], keys.at[1 - core], k_ss.at[0], k_rs.at[0], role, me
            ).wait_recv()
            remote(
                values_in.at[:, :, mate_keys], values.at[1 - core], k_ss.at[1], k_rs.at[1], role, me
            ).wait_recv()
        else:
            wait_query(slot)
            wait_query(slot + 1)
        lanes = pl.ds(pl.multiple_of(local * HEAD_SIZE, HEAD_SIZE), HEAD_SIZE)
        query = jnp.concatenate(
            [
                q_all[slot + part, :, j * HEAD_SIZE : (j + 1) * HEAD_SIZE].astype(f32)
                for part in range(2)
                for j in range(own_heads)
            ],
            axis=0,
        ).astype(bf16)
        key = keys[:, :, :, lanes].reshape(slots, HEAD_SIZE)
        value = values[:, :, :, lanes].reshape(slots, HEAD_SIZE)
        scores = lax.dot_general(query, key, (((1,), (1,)), ((), ())), preferred_element_type=f32)
        scores = (scores * scale).reshape(group, rows, slots) + bias[...][None]
        scores = scores.reshape(group * rows, slots)
        top = jnp.max(scores, axis=1, keepdims=True)
        top = jnp.maximum(top, DEAD).astype(bf16).astype(f32)
        probs = jnp.exp(scores - top).astype(bf16)
        both = jnp.dot(
            probs, jnp.concatenate([value, ones], axis=1), preferred_element_type=f32
        )
        weighted = both[:, :HEAD_SIZE]
        total = both[:, HEAD_SIZE:]
        total_high = total.astype(bf16).astype(f32)
        total_low = total - total_high
        for part in range(2):
            stats = jnp.zeros((rows, HEAD_SIZE), f32)
            for j in range(own_heads):
                at = (part * own_heads + j) * rows
                stats = jnp.where(lane == j, top[at : at + rows], stats)
                stats = jnp.where(lane == own_heads + j, total_high[at : at + rows], stats)
                stats = jnp.where(lane == 2 * own_heads + j, total_low[at : at + rows], stats)
            first = part * own_heads * rows
            b_send[slot + part] = jnp.concatenate(
                [weighted[first : first + own_heads * rows], stats], axis=0
            ).astype(bf16)
        for part in range(2):
            to = core * half + slot + part
            copy = remote(
                b_send.at[slot + part], b_recv.at[chip], b_ss.at[2 * i + part], b_rs, role, to
            )
            if i == 0:

                @pl.when(to != me)
                def _(copy=copy):
                    copy.start()

                @pl.when(to == me)
                def _(part=part):
                    b_recv[chip] = b_send[slot + part]

            else:
                copy.start()

    for copy in loads[4:9]:
        copy.wait()
    own_query = q_own[...].astype(f32)
    fresh = []
    for u in range(DECODE_STEPS):
        fresh_key = fresh_keys[u].astype(f32)
        fresh.append(
            [
                jnp.where(
                    u <= step,
                    jnp.sum(
                        own_query[:, j * HEAD_SIZE : (j + 1) * HEAD_SIZE] * fresh_key,
                        axis=1,
                        keepdims=True,
                    )
                    * scale,
                    LOW,
                )
                for j in range(own_heads)
            ]
        )

    @pl.when(core == side)
    def _():
        landed(b_recv.at[pl.ds(0, chips - 1)], b_rs)

    @pl.when(core != side)
    def _():
        landed(b_recv, b_rs)

    stats = [b_recv[s, own_heads * rows :, :].astype(f32) for s in range(chips)]
    top = functools.reduce(jnp.maximum, stats)
    tops = [
        functools.reduce(
            jnp.maximum, [fresh[u][j] for u in range(DECODE_STEPS)], top[:, j : j + 1]
        )
        for j in range(own_heads)
    ]
    numerator = [jnp.zeros((rows, HEAD_SIZE), f32) for _ in range(own_heads)]
    denominator = [jnp.zeros((rows, 1), f32) for _ in range(own_heads)]
    for j in range(own_heads):
        for u in range(DECODE_STEPS):
            weight = jnp.where(u <= step, jnp.exp(fresh[u][j] - tops[j]), 0.0)
            numerator[j] += weight * fresh_values[u].astype(f32)
            denominator[j] += weight
    for s in range(chips):
        part = b_recv[s, : own_heads * rows, :].astype(f32)
        for j in range(own_heads):
            factor = jnp.exp(stats[s][:, j : j + 1] - tops[j])
            numerator[j] += factor * part[j * rows : (j + 1) * rows]
            at = own_heads + j
            denominator[j] += factor * (
                stats[s][:, at : at + 1] + stats[s][:, at + own_heads : at + own_heads + 1]
            )
    attended = jnp.concatenate(
        [numerator[j] / denominator[j] for j in range(own_heads)], axis=1
    ).astype(bf16)

    loads[9].wait()
    block = 4
    for i in range(n // block - 1, -1, -1):
        base = flip(me // block, i, n // block) * block
        out = jnp.dot(
            attended,
            wo_buf[:, pl.ds(pl.multiple_of(base * width, 128), block * width)],
            preferred_element_type=f32,
        )
        for j in range(block):
            c_send[base + j] = out[:, j * width : (j + 1) * width].astype(bf16)
        for j in range(block):
            to = base + j
            copy = remote(c_send.at[to], c_recv.at[me], c_ss, c_rs, role, to)
            if i == 0:

                @pl.when(to != me)
                def _(copy=copy):
                    copy.start()

            else:
                copy.start()
    state = resid[...].astype(f32)
    c_recv[me] = c_send[me]

    landed(c_recv.at[pl.ds(0, n - 1)], c_rs)
    for s in range(n):
        state += c_recv[s].astype(f32)

    def slot_of(from_role, place):
        return 2 * place + 1 - from_role

    mine = slot_of(role, me)
    x_all[mine] = (state * gain[...]).astype(bf16)

    def x_copy(slot, rs, ss, to_role, to):
        return remote(x_all.at[slot], x_all.at[slot], ss, rs, to_role, to)

    for i in range(chips - 1, -1, -1):
        to = 2 * flip(chip, i, chips) + core
        x_copy(mine, x_rs.at[mine], d_ss, 1 - role, to).start()
        if i:
            x_copy(mine, x_rs.at[mine], d_ss, role, to).start()
    x_copy(mine, x_rs.at[mine], d_ss, role, mate).start()

    diagonal = lax.broadcasted_iota(jnp.int32, (rows, HEAD_SIZE), 0)
    square = jnp.sum(state * state, axis=1, keepdims=True)
    s_send[...] = jnp.sum(jnp.where(diagonal == lane, square, 0.0), axis=0, keepdims=True)
    own_stat = role * n + me
    for i in range(n - 1, -1, -1):
        to = flip(me, i, n)
        remote(s_send, s_recv.at[own_stat], s_ss, s_rs, 1 - role, to).start()
        if i:
            remote(s_send, s_recv.at[own_stat], s_ss, s_rs, role, to).start()
    s_recv[own_stat] = s_send[...]

    @pl.loop(0, n)
    def _(p):
        head_copy(p).wait()

    def wait_x(slot):
        x_copy(slot, x_rs.at[slot], d_ss, role, me).wait_recv()

    def chunk(place, start):
        x = jnp.concatenate(
            [x_all[2 * place].astype(f32), x_all[2 * place + 1].astype(f32)], axis=0
        ).astype(bf16)
        lanes = pl.ds(pl.multiple_of(place * width, 128), width)
        for t in range(tiles):
            size = min(TILE, kept - t * TILE)
            y = lax.dot_general(
                x,
                head_buf[t * TILE : t * TILE + size, lanes],
                (((1,), (1,)), ((), ())),
                preferred_element_type=f32,
            )
            if start:
                acc[t, :, :size] = y
            else:
                acc[t, :, :size] += y

    def take(slot):
        wait_x(slot)
        x_copy(slot, x_rs.at[slot], f_ss, role, mate).start()

    take(slot_of(1 - role, me))
    chunk(me, True)

    @pl.loop(1, chips)
    def _(i):
        place = 2 * flip(chip, i, chips) + core
        take(2 * place)
        take(2 * place + 1)
        chunk(place, False)
        place = 2 * flip(chip, i - 1, chips) + 1 - core
        wait_x(2 * place)
        wait_x(2 * place + 1)
        chunk(place, False)

    last = 2 * flip(chip, chips - 1, chips) + 1 - core
    wait_x(2 * last)
    wait_x(2 * last + 1)
    chunk(last, False)

    landed(s_recv.at[pl.ds(0, 2 * n - 1)], s_rs)
    inverse = []
    for t in range(DECODE_STEPS):
        square = functools.reduce(jnp.add, [s_recv[(1 - t) * n + s] for s in range(n)])
        factor = lax.rsqrt(square / (n * width) + 1e-05)
        inverse.append(
            jnp.sum(jnp.where(diagonal == lane, factor, 0.0), axis=1, keepdims=True)
        )
    own_inverse = jnp.where(role == 0, inverse[1], inverse[0])
    inverse = jnp.concatenate(inverse, axis=0)
    n_send[...] = (state * own_inverse * gain[...]).astype(bf16)
    n_copy = remote(n_send, n_recv, n_sems.at[0], n_sems.at[1], 1 - role, me)
    n_copy.start()

    action_rows = lax.broadcasted_iota(jnp.int32, (2 * rows, 1), 0)
    action = jnp.zeros((2 * rows, 1), jnp.int32)
    for t in range(DECODE_STEPS):
        for b in range(rows):
            action = jnp.where(action_rows == t * rows + b, actions[t, b], action)
    wanted = action - (me * vocab + first_row)
    twice = role * (2 * kept - vocab)
    tile_ids = lax.broadcasted_iota(jnp.int32, (2 * rows, TILE), 1)
    largest = jnp.full((2 * rows, 1), LOW, f32)
    logits = []
    for t in range(tiles):
        size = min(TILE, kept - t * TILE)
        tile = acc[t, :, :size] * inverse
        if t == 0:
            tile = jnp.where(tile_ids[:, :size] < twice, LOW, tile)
        logits.append(tile)
    whole = [tile for tile in logits if tile.shape[1] == TILE]
    largest = jnp.max(functools.reduce(jnp.maximum, whole), axis=1, keepdims=True)
    for tile in logits:
        if tile.shape[1] != TILE:
            largest = jnp.maximum(largest, jnp.max(tile, axis=1, keepdims=True))
    exp_sum = jnp.zeros((2 * rows, 1), f32)
    target = jnp.zeros((2 * rows, 1), f32)
    whole_sum = jnp.zeros((2 * rows, TILE), f32)
    whole_target = jnp.zeros((2 * rows, TILE), f32)
    for t, tile in enumerate(logits):
        size = tile.shape[1]
        here = tile_ids[:, :size] + t * TILE == wanted
        if t == 0:
            here = here & (tile_ids[:, :size] >= twice)
        power = jnp.exp(tile - largest)
        hit = jnp.where(here, tile, 0.0)
        if size == TILE:
            whole_sum += power
            whole_target += hit
        else:
            exp_sum += jnp.sum(power, axis=1, keepdims=True)
            target += jnp.sum(hit, axis=1, keepdims=True)
    exp_sum += jnp.sum(whole_sum, axis=1, keepdims=True)
    target += jnp.sum(whole_target, axis=1, keepdims=True)
    for t in range(DECODE_STEPS):
        part = slice(t * rows, (t + 1) * rows)
        packed = jnp.where(lane == diagonal, largest[part], 0.0)
        packed = jnp.where(lane == diagonal + rows, exp_sum[part], packed)
        packed = jnp.where(lane == diagonal + 2 * rows, target[part], packed)
        e_send[t] = jnp.sum(packed, axis=0, keepdims=True)
    for i in range(n - 1, -1, -1):
        to = flip(me, i, n)
        remote(e_send.at[1 - role], e_recv.at[own_stat], e_ss, e_rs, 1 - role, to).start()
        if i:
            remote(e_send.at[role], e_recv.at[own_stat], e_ss, e_rs, role, to).start()
    e_recv[own_stat] = e_send[role]

    n_copy.wait_recv()
    out_copy = pltpu.make_async_copy(n_recv, normed.at[0], n_sems.at[2])
    out_copy.start()
    n_copy.wait_send()
    for i in range(1, chips):
        remote(q_own, q_all.at[own_slot], q_ss.at[i], q_rs.at[own_slot], role, me).wait_send()

    @pl.when(core != side)
    def _():
        remote(q_own, q_all.at[own_slot], q_ss.at[0], q_rs.at[own_slot], role, mate).wait_send()

    key_swap.wait_send()
    value_swap.wait_send()
    for i in range(near):
        for part in range(2):
            copy = remote(
                b_send.at[0], b_recv.at[chip], b_ss.at[2 * i + part], b_rs, role, me
            )
            if i == 0:

                @pl.when(core * half + 2 * (chip % near) + part != me)
                def _(copy=copy):
                    copy.wait_send()

            else:
                copy.wait_send()
    landed(c_send.at[pl.ds(0, n - 1)], c_ss)
    landed(x_all.at[pl.ds(0, n)], d_ss)
    landed(x_all.at[pl.ds(0, n - 1)], f_ss)
    landed(s_recv.at[pl.ds(0, 2 * n - 1)], s_ss)

    landed(e_recv.at[pl.ds(0, 2 * n - 1)], e_rs)
    got = [e_recv[s] for s in range(2 * n)]
    top = functools.reduce(jnp.maximum, got)
    exp_sum = jnp.zeros((1, HEAD_SIZE), f32)
    target = jnp.zeros((1, HEAD_SIZE), f32)
    stack = jnp.concatenate(got, axis=0)
    factor = pltpu.roll(jnp.exp(stack - top), rows, 1)
    exp_sum = jnp.sum(stack * factor, axis=0, keepdims=True)
    target = jnp.sum(stack, axis=0, keepdims=True)
    exp_sum = pltpu.roll(exp_sum, HEAD_SIZE - rows, 1)
    target = pltpu.roll(target, HEAD_SIZE - 2 * rows, 1)
    log_probs[...] = (target - top - jnp.log(exp_sum))[:, :rows]
    landed(e_recv.at[pl.ds(0, 2 * n - 1)], e_ss)
    out_copy.wait()


def fused(
    queries,
    step_token_keys,
    step_token_values,
    stored_key_cache,
    stored_value_cache,
    lengths,
    wo_sides,
    gain_sides,
    head,
    resid,
    actions,
):
    tp = lax.axis_size("tp")
    n = lax.axis_size("grp") * tp
    rows = lengths.shape[0]
    width = resid.shape[2]
    heads = width // HEAD_SIZE
    kept = -(-head.shape[1] // 16) * 8
    tiles = -(-kept // TILE)
    shard = stored_key_cache.shape[1]
    slots = 2 * rows * shard
    half_keys = stored_key_cache.shape[2] // 2
    bf16, f32 = jnp.bfloat16, jnp.float32
    vmem = pl.BlockSpec(memory_space=pltpu.VMEM)
    hbm = pl.BlockSpec(memory_space=pl.ANY)
    message = heads * rows + rows
    dma = pltpu.SemaphoreType.DMA
    return pl.pallas_call(
        functools.partial(fused_kernel, n, tp),
        out_shape=(
            jax.ShapeDtypeStruct((1, rows), f32),
            jax.ShapeDtypeStruct((1, rows, width), bf16),
        ),
        in_specs=[hbm] * 11,
        out_specs=(vmem, hbm),
        scratch_shapes=[
            pltpu.VMEM((rows, width), bf16),
            pltpu.VMEM((DECODE_STEPS, rows, HEAD_SIZE), bf16),
            pltpu.VMEM((DECODE_STEPS, rows, HEAD_SIZE), bf16),
            pltpu.SMEM((rows,), jnp.int32),
            pltpu.SMEM((DECODE_STEPS, rows), jnp.int32),
            pltpu.VMEM((1, width), f32),
            pltpu.VMEM((rows, width), bf16),
            pltpu.VMEM((2, rows, shard, half_keys), bf16),
            pltpu.VMEM((2, rows, shard, half_keys), bf16),
            pltpu.VMEM(wo_sides.shape[1:], bf16),
            pltpu.VMEM((kept, head.shape[0]), bf16),
            pltpu.VMEM((rows, slots), f32),
            pltpu.VMEM((n // 2, rows, width), bf16),
            pltpu.VMEM((n // 2, message, HEAD_SIZE), bf16),
            pltpu.VMEM((n // 2, message, HEAD_SIZE), bf16),
            pltpu.VMEM((n, rows, width), bf16),
            pltpu.VMEM((n, rows, width), bf16),
            pltpu.VMEM((2 * n, rows, width), bf16),
            pltpu.VMEM((1, HEAD_SIZE), f32),
            pltpu.VMEM((2 * n, 1, HEAD_SIZE), f32),
            pltpu.VMEM((tiles, 2 * rows, TILE), f32),
            pltpu.VMEM((rows, width), bf16),
            pltpu.VMEM((rows, width), bf16),
            pltpu.VMEM((2, 1, HEAD_SIZE), f32),
            pltpu.VMEM((2 * n, 1, HEAD_SIZE), f32),
            dma((10,)),
            dma((n,)),
            dma((n // 2,)),
            dma((n // 2,)),
            dma((2,)),
            dma((2,)),
            dma((n // 2,)),
            dma,
            dma,
            dma,
            dma,
            dma,
            dma((2 * n,)),
            dma,
            dma,
            dma((3,)),
            dma,
            dma,
        ],
        compiler_params=pltpu.CompilerParams(
            collective_id=0, has_side_effects=True, vmem_limit_bytes=60 * 1024 * 1024
        ),
    )(
        queries,
        step_token_keys,
        step_token_values,
        stored_key_cache,
        stored_value_cache,
        lengths,
        gain_sides,
        resid,
        actions,
        wo_sides,
        head.T,
    )


def on_device(*args):
    queries, lengths, head = args[0], args[5], args[8]
    tp = lax.axis_size("tp")
    n = lax.axis_size("grp") * tp
    width = queries.shape[2]
    group = QUERY_HEADS // KEY_VALUE_HEADS
    whole_heads = width % HEAD_SIZE == 0 and 2 * (width // HEAD_SIZE) == group
    powers = n & (n - 1) == 0 and n >= 8 and tp % 2 == 0 and n // 2 == KEY_VALUE_HEADS
    fits = lax.axis_size("role") == 2 and powers and lengths.shape[0] == 8
    if whole_heads and fits and head.shape[0] == n * width and head.shape[1] % 8 == 0:
        return fused(*args)
    return plain(*args)


def solution(mesh):
    in_specs = (
        P(None, None, ("grp", "tp")),
        P(),
        P(),
        P(None, ("grp", "tp"), None),
        P(None, ("grp", "tp"), None),
        P(),
        P("role", ("grp", "tp"), None),
        P("role", ("grp", "tp")),
        P(None, ("grp", "tp")),
        P(None, None, ("grp", "tp")),
        P(),
    )
    out_specs = (P("role", None), P("role", None, ("grp", "tp")))
    return jax.shard_map(
        on_device, mesh=mesh, in_specs=in_specs, out_specs=out_specs, check_vma=False
    )
```

```python
import functools
import math

import jax
import jax.numpy as jnp
from jax import lax
from jax.experimental import pallas as pl
from jax.experimental.pallas import tpu as pltpu
from jax.sharding import PartitionSpec as P

D = 8192
QUERY_HEADS = 64
KEY_VALUE_HEADS = 8
HEAD_SIZE = 128
DECODE_STEPS = 2


def swap_sides(value):
    return lax.ppermute(value, "role", [(0, 1), (1, 0)])


def plain(
    queries,
    step_token_keys,
    step_token_values,
    stored_key_cache,
    stored_value_cache,
    lengths,
    wo_sides,
    gain_sides,
    head,
    resid,
    actions,
):
    both = ("grp", "tp")
    place = lax.axis_index(both)
    step = 1 - lax.axis_index("role")
    count_of_rows = lengths.shape[0]
    shard_length = stored_key_cache.shape[1]
    query_group_width = QUERY_HEADS // KEY_VALUE_HEADS
    logit_scale = 1.0 / math.sqrt(HEAD_SIZE)
    query_matrix = lax.all_gather(
        lax.dynamic_index_in_dim(queries, step, 0, keepdims=False), both, axis=1, tiled=True
    )
    positions = place * shard_length + jnp.arange(shard_length, dtype=jnp.int32)
    valid = positions[None, :] < lengths[:, None]
    masking = valid[:, None, None, :]
    cache_shape = (count_of_rows, shard_length, KEY_VALUE_HEADS, HEAD_SIZE)
    prior_keys = stored_key_cache.reshape(cache_shape)
    prior_values = stored_value_cache.reshape(cache_shape)
    step_shape = (DECODE_STEPS, count_of_rows, KEY_VALUE_HEADS, HEAD_SIZE)
    incoming_keys = step_token_keys.astype(jnp.float32).reshape(step_shape)
    incoming_values = step_token_values.astype(jnp.float32).reshape(step_shape)
    current_query = query_matrix.reshape(
        count_of_rows, KEY_VALUE_HEADS, query_group_width, HEAD_SIZE
    )
    scores = (
        jnp.einsum("rkgd,rskd->rkgs", current_query, prior_keys, preferred_element_type=jnp.float32)
        * logit_scale
    )
    scores = jnp.where(masking, scores, -1e30)
    fresh_live = jnp.arange(DECODE_STEPS, dtype=jnp.int32) <= step
    fresh_scores = (
        jnp.einsum("rkgd,trkd->rkgt", current_query.astype(jnp.float32), incoming_keys)
        * logit_scale
    )
    fresh_scores = jnp.where(fresh_live, fresh_scores, -1e30)
    fresh_highest = jnp.max(fresh_scores, axis=-1)
    overall = lax.pmax(jnp.maximum(jnp.max(scores, axis=-1), fresh_highest), both)
    cache_probs = jnp.exp(scores - overall[..., None]) * masking
    fresh_probs = jnp.exp(fresh_scores - overall[..., None]) * fresh_live
    fresh_probs = fresh_probs * (place == 0)
    totals = jnp.sum(cache_probs, axis=-1) + jnp.sum(fresh_probs, axis=-1)
    weighted = jnp.einsum(
        "rkgs,rskd->rkgd", cache_probs, prior_values.astype(jnp.float32)
    ) + jnp.einsum("rkgt,trkd->rkgd", fresh_probs, incoming_values)
    features = QUERY_HEADS * HEAD_SIZE
    mixed = lax.psum_scatter(
        weighted.reshape(count_of_rows, features), both, scatter_dimension=1, tiled=True
    )
    totals = lax.psum(totals.reshape(count_of_rows, QUERY_HEADS), both)
    feature_rows = wo_sides.shape[1]
    own_heads = (place * feature_rows + jnp.arange(feature_rows)) // HEAD_SIZE
    own_part = (mixed / jnp.take(totals, own_heads, axis=1)).astype(jnp.bfloat16)
    branch_out = lax.psum_scatter(
        jnp.dot(own_part, wo_sides[0], preferred_element_type=jnp.float32),
        both,
        scatter_dimension=1,
        tiled=True,
    )
    resid_now = lax.dynamic_index_in_dim(resid, step, 0, keepdims=False)
    state = resid_now.astype(jnp.float32) + branch_out
    square_sum = lax.psum(jnp.sum(state * state, axis=-1), both)
    normed_now = (
        state * lax.rsqrt(square_sum[:, None] / D + 1e-05) * gain_sides[0][None, :]
    ).astype(jnp.bfloat16)
    logits = jnp.dot(
        lax.all_gather(normed_now, both, axis=1, tiled=True),
        head,
        preferred_element_type=jnp.float32,
    )
    local_highest = jnp.max(logits, axis=-1)
    action_now = lax.dynamic_index_in_dim(actions, step, 0, keepdims=False)
    head_width = head.shape[1]
    vocab_ids = place * head_width + jnp.arange(head_width, dtype=jnp.int32)
    is_target = vocab_ids[None, :] == action_now[:, None]
    target = jnp.sum(jnp.where(is_target, logits, 0.0), axis=-1)
    exp_sum = jnp.sum(jnp.exp(logits - local_highest[:, None]), axis=-1)
    parts = lax.all_gather(jnp.stack([local_highest, exp_sum, target]), both)
    largest = jnp.max(parts[:, 0], axis=0)
    exp_sum = jnp.sum(parts[:, 1] * jnp.exp(parts[:, 0] - largest[None]), axis=0)
    prob_now = jnp.sum(parts[:, 2], axis=0) - largest - jnp.log(exp_sum)
    return (swap_sides(prob_now)[None], swap_sides(normed_now)[None])


LOW = -1e30
DEAD = -1e29
TILE = 256
SINGLE = 3
TURNS = (3, 3, 5, 3, 2)
MESH = pl.DeviceIdType.MESH


def fused_kernel(
    n,
    tp,
    queries,
    token_keys,
    token_values,
    keys_in,
    values_in,
    lengths_in,
    gain_in,
    resid_in,
    actions_in,
    wo,
    head,
    log_probs,
    normed,
    q_own,
    fresh_keys,
    fresh_values,
    lengths,
    actions,
    gain,
    resid,
    keys,
    values,
    wo_buf,
    near_head,
    far_head,
    turned,
    bias,
    q_all,
    b_send,
    b_recv,
    c_send,
    c_recv,
    x_all,
    s_send,
    s_recv,
    acc,
    n_send,
    n_recv,
    e_send,
    e_recv,
    in_sems,
    head_sems,
    q_ss,
    q_rs,
    k_ss,
    k_rs,
    b_ss,
    b_rs,
    c_ss,
    c_rs,
    d_ss,
    f_ss,
    x_rs,
    s_ss,
    s_rs,
    n_sems,
    e_ss,
    e_rs,
):
    role = lax.axis_index("role")
    me = lax.axis_index("grp") * tp + lax.axis_index("tp")
    core = me % 2
    chip = me // 2
    mate = me + 1 - 2 * core
    chips = n // 2
    near = chips // 2
    half = n // 2
    side = chip // near
    step = 1 - role
    rows = resid.shape[0]
    width = resid.shape[1]
    shard = keys.shape[2]
    half_keys = keys.shape[3]
    own_heads = width // HEAD_SIZE
    group = QUERY_HEADS // KEY_VALUE_HEADS
    slots = 2 * rows * shard
    vocab = head.shape[0]
    kept = -(-vocab // 16) * 8
    tiles = acc.shape[0]
    scale = 1.0 / math.sqrt(HEAD_SIZE)
    f32 = jnp.float32
    bf16 = jnp.bfloat16

    def flip(index, by, size):
        out = index
        bit = 1
        while bit < size:
            if isinstance(by, int):
                if by // bit % 2:
                    out = out + bit - 2 * bit * (index // bit % 2)
            else:
                out = out + (by // bit % 2) * (bit - 2 * bit * (index // bit % 2))
            bit *= 2
        return out

    def remote(src, dst, ss, rs, to_role, place):
        return pltpu.make_async_remote_copy(
            src_ref=src,
            dst_ref=dst,
            send_sem=ss,
            recv_sem=rs,
            device_id=(to_role, place // tp, place % tp),
            device_id_type=MESH,
        )

    def landed(ref, sem):
        pltpu.make_async_copy(ref, ref, sem).wait()

    own_keys = pl.ds(pl.multiple_of(core * half_keys, 128), half_keys)
    mate_keys = pl.ds(pl.multiple_of((1 - core) * half_keys, 128), half_keys)
    chip_lanes = pl.ds(pl.multiple_of(chip * HEAD_SIZE, HEAD_SIZE), HEAD_SIZE)
    loads = [
        pltpu.make_async_copy(src, dst, in_sems.at[i])
        for i, (src, dst) in enumerate(
            [
                (queries.at[step], q_own),
                (lengths_in, lengths),
                (keys_in.at[:, :, own_keys], keys.at[core]),
                (values_in.at[:, :, own_keys], values.at[core]),
                (token_keys.at[:, :, chip_lanes], fresh_keys),
                (token_values.at[:, :, chip_lanes], fresh_values),
                (resid_in.at[step], resid),
                (gain_in, gain),
                (actions_in, actions),
                (wo.at[0], wo_buf),
            ]
        )
    ]
    loads[0].start()
    barrier = pltpu.get_barrier_semaphore()
    for i in range(1, 2 * n):
        other = (role * n + me + i) % (2 * n)
        pl.semaphore_signal(
            barrier,
            inc=1,
            device_id=(other // n, other % n // tp, other % tp),
            device_id_type=MESH,
        )
    for copy in loads[1:-1]:
        copy.start()
    first_row = pl.multiple_of(role * (vocab - kept), 8)

    def direct(i):
        return 2 * flip(chip, i, chips) + core

    def relayed(i):
        return 2 * flip(chip, i, chips) + 1 - core

    def head_copy(place, buf, i, sem):
        lanes = pl.ds(pl.multiple_of(place * width, 128), width)
        return pltpu.make_async_copy(
            head.at[pl.ds(first_row, kept), lanes], buf.at[i, pl.ds(0, kept), :], head_sems.at[sem]
        )

    def near_copy(i):
        return head_copy(direct(i), near_head, i, i)

    def far_copy(i):
        return head_copy(relayed(i), far_head, i, chips + i)

    @pl.loop(0, TURNS[0])
    def _(i):
        near_copy(i).start()

    loads[-1].start()

    @pl.loop(TURNS[0], chips)
    def _(i):
        near_copy(i).start()

    @pl.loop(0, chips)
    def _(i):
        far_copy(i).start()

    pl.semaphore_wait(barrier, 2 * n - 1)
    loads[0].wait()

    own_slot = me % half
    for i in range(chips - 1, 0, -1):
        to = 2 * flip(chip, i, chips) + side
        remote(q_own, q_all.at[own_slot], q_ss.at[i], q_rs.at[own_slot], role, to).start()

    @pl.when(core != side)
    def _():
        remote(q_own, q_all.at[own_slot], q_ss.at[0], q_rs.at[own_slot], role, mate).start()

    @pl.when(core == side)
    def _():
        q_all[own_slot] = q_own[...]

    key_swap = remote(
        keys_in.at[:, :, mate_keys], keys.at[core], k_ss.at[0], k_rs.at[0], role, mate
    )
    value_swap = remote(
        values_in.at[:, :, mate_keys], values.at[core], k_ss.at[1], k_rs.at[1], role, mate
    )
    key_swap.start()
    value_swap.start()

    loads[1].wait()
    row_ids = lax.broadcasted_iota(jnp.int32, (rows, slots), 0)
    col_ids = lax.broadcasted_iota(jnp.int32, (rows, slots), 1)
    limit = jnp.zeros((rows, slots), jnp.int32)
    for b in range(rows):
        limit = jnp.where(row_ids == b, lengths[b], limit)
    origin = col_ids // (rows * shard)
    place_ids = (2 * chip + origin) * shard + col_ids % shard
    live = (col_ids // shard % rows == row_ids) & (place_ids < limit)
    bias[...] = jnp.where(live, 0.0, LOW)

    def turn_one(copy, source, target, i, j):
        copy(i).wait()
        for t in range(tiles):
            size = min(TILE, kept - t * TILE)
            tile = source[i, t * TILE : t * TILE + size, :].T
            for k in range(width // TILE):
                target[j, t * TILE : (t + 1) * TILE, k * TILE : k * TILE + size] = tile[
                    k * TILE : (k + 1) * TILE
                ]

    def turn(window):
        first = sum(TURNS[:window])
        last = first + TURNS[window]

        @pl.loop(min(first, chips), min(last, chips))
        def _(i):
            turn_one(near_copy, near_head, turned, i, i)

        @pl.loop(max(first - chips, 0), max(last - chips, 0))
        def _(i):
            turn_one(far_copy, far_head, near_head, i, i)

    turn(0)
    loads[2].wait()
    loads[3].wait()
    ones = jnp.ones((slots, HEAD_SIZE), bf16)
    lane = lax.broadcasted_iota(jnp.int32, (rows, HEAD_SIZE), 1)

    def wait_query(slot):
        remote(q_own, q_all.at[slot], q_ss.at[0], q_rs.at[slot], role, me).wait_recv()

    for i in range(near):
        local = flip(chip % near, i, near)
        slot = 2 * local
        if i == 0:

            @pl.when(core == side)
            def _():
                wait_query(mate % half)

            @pl.when(core != side)
            def _():
                wait_query(slot)
                wait_query(slot + 1)

            remote(
                keys_in.at[:, :, mate_keys], keys.at[1 - core], k_ss.at[0], k_rs.at[0], role, me
            ).wait_recv()
            remote(
                values_in.at[:, :, mate_keys], values.at[1 - core], k_ss.at[1], k_rs.at[1], role, me
            ).wait_recv()
        else:
            wait_query(slot)
            wait_query(slot + 1)
        lanes = pl.ds(pl.multiple_of(local * HEAD_SIZE, HEAD_SIZE), HEAD_SIZE)
        query = jnp.concatenate(
            [
                q_all[slot + part, :, j * HEAD_SIZE : (j + 1) * HEAD_SIZE].astype(f32)
                for part in range(2)
                for j in range(own_heads)
            ],
            axis=0,
        ).astype(bf16)
        key = keys[:, :, :, lanes].reshape(slots, HEAD_SIZE)
        value = values[:, :, :, lanes].reshape(slots, HEAD_SIZE)
        scores = lax.dot_general(query, key, (((1,), (1,)), ((), ())), preferred_element_type=f32)
        scores = (scores * scale).reshape(group, rows, slots) + bias[...][None]
        scores = scores.reshape(group * rows, slots)
        top = jnp.max(scores, axis=1, keepdims=True)
        top = jnp.maximum(top, DEAD).astype(bf16).astype(f32)
        probs = jnp.exp(scores - top).astype(bf16)
        both = jnp.dot(
            probs, jnp.concatenate([value, ones], axis=1), preferred_element_type=f32
        )
        weighted = both[:, :HEAD_SIZE]
        total = both[:, HEAD_SIZE:]
        total_high = total.astype(bf16).astype(f32)
        total_low = total - total_high
        for part in range(2):
            stats = jnp.zeros((rows, HEAD_SIZE), f32)
            for j in range(own_heads):
                at = (part * own_heads + j) * rows
                stats = jnp.where(lane == j, top[at : at + rows], stats)
                stats = jnp.where(lane == own_heads + j, total_high[at : at + rows], stats)
                stats = jnp.where(lane == 2 * own_heads + j, total_low[at : at + rows], stats)
            first = part * own_heads * rows
            b_send[slot + part] = jnp.concatenate(
                [weighted[first : first + own_heads * rows], stats], axis=0
            ).astype(bf16)
        for part in range(2):
            to = core * half + slot + part
            copy = remote(
                b_send.at[slot + part], b_recv.at[chip], b_ss.at[2 * i + part], b_rs, role, to
            )
            if i == 0:

                @pl.when(to != me)
                def _(copy=copy):
                    copy.start()

                @pl.when(to == me)
                def _(part=part):
                    b_recv[chip] = b_send[slot + part]

            else:
                copy.start()

    for copy in loads[4:9]:
        copy.wait()
    own_query = q_own[...].astype(f32)
    fresh = []
    for u in range(DECODE_STEPS):
        fresh_key = fresh_keys[u].astype(f32)
        fresh.append(
            [
                jnp.where(
                    u <= step,
                    jnp.sum(
                        own_query[:, j * HEAD_SIZE : (j + 1) * HEAD_SIZE] * fresh_key,
                        axis=1,
                        keepdims=True,
                    )
                    * scale,
                    LOW,
                )
                for j in range(own_heads)
            ]
        )

    turn(1)

    @pl.when(core == side)
    def _():
        landed(b_recv.at[pl.ds(0, chips - 1)], b_rs)

    @pl.when(core != side)
    def _():
        landed(b_recv, b_rs)

    stats = [b_recv[s, own_heads * rows :, :].astype(f32) for s in range(chips)]
    top = functools.reduce(jnp.maximum, stats)
    tops = [
        functools.reduce(
            jnp.maximum, [fresh[u][j] for u in range(DECODE_STEPS)], top[:, j : j + 1]
        )
        for j in range(own_heads)
    ]
    numerator = [jnp.zeros((rows, HEAD_SIZE), f32) for _ in range(own_heads)]
    denominator = [jnp.zeros((rows, 1), f32) for _ in range(own_heads)]
    for j in range(own_heads):
        for u in range(DECODE_STEPS):
            weight = jnp.where(u <= step, jnp.exp(fresh[u][j] - tops[j]), 0.0)
            numerator[j] += weight * fresh_values[u].astype(f32)
            denominator[j] += weight
    for s in range(chips):
        part = b_recv[s, : own_heads * rows, :].astype(f32)
        for j in range(own_heads):
            factor = jnp.exp(stats[s][:, j : j + 1] - tops[j])
            numerator[j] += factor * part[j * rows : (j + 1) * rows]
            at = own_heads + j
            denominator[j] += factor * (
                stats[s][:, at : at + 1] + stats[s][:, at + own_heads : at + own_heads + 1]
            )
    attended = jnp.concatenate(
        [numerator[j] / denominator[j] for j in range(own_heads)], axis=1
    ).astype(bf16)

    loads[9].wait()
    block = 4
    for i in range(n // block - 1, -1, -1):
        base = flip(me // block, i, n // block) * block
        out = jnp.dot(
            attended,
            wo_buf[:, pl.ds(pl.multiple_of(base * width, 128), block * width)],
            preferred_element_type=f32,
        )
        for j in range(block):
            c_send[base + j] = out[:, j * width : (j + 1) * width].astype(bf16)
        for j in range(block):
            to = base + j
            copy = remote(c_send.at[to], c_recv.at[me], c_ss, c_rs, role, to)
            if i == 0:

                @pl.when(to != me)
                def _(copy=copy):
                    copy.start()

            else:
                copy.start()
    state = resid[...].astype(f32)
    c_recv[me] = c_send[me]

    turn(2)
    landed(c_recv.at[pl.ds(0, n - 1)], c_rs)
    for s in range(n):
        state += c_recv[s].astype(f32)

    def slot_of(from_role, place):
        return 2 * place + 1 - from_role

    mine = slot_of(role, me)
    x_all[mine] = (state * gain[...]).astype(bf16)

    def x_copy(slot, rs, ss, to_role, to):
        return remote(x_all.at[slot], x_all.at[slot], ss, rs, to_role, to)

    for i in range(chips):
        to = 2 * flip(chip, i, chips) + core
        x_copy(mine, x_rs.at[mine], d_ss, 1 - role, to).start()
        if i == 0:
            to = mate
        x_copy(mine, x_rs.at[mine], d_ss, role, to).start()

    diagonal = lax.broadcasted_iota(jnp.int32, (rows, HEAD_SIZE), 0)
    square = jnp.sum(state * state, axis=1, keepdims=True)
    s_send[...] = jnp.sum(jnp.where(diagonal == lane, square, 0.0), axis=0, keepdims=True)
    own_stat = role * n + me
    for i in range(n - 1, -1, -1):
        to = flip(me, i, n)
        remote(s_send, s_recv.at[own_stat], s_ss, s_rs, 1 - role, to).start()
        if i:
            remote(s_send, s_recv.at[own_stat], s_ss, s_rs, role, to).start()
    s_recv[own_stat] = s_send[...]

    turn(3)

    def wait_x(slot):
        x_copy(slot, x_rs.at[slot], d_ss, role, me).wait_recv()

    def features(place):
        return jnp.concatenate(
            [x_all[2 * place].astype(f32), x_all[2 * place + 1].astype(f32)], axis=0
        ).astype(bf16)

    def turned_dot(x, ref, i, t, size):
        return functools.reduce(
            jnp.add,
            [
                jnp.dot(
                    x[:, k * TILE : (k + 1) * TILE],
                    ref[i, t * TILE : (t + 1) * TILE, k * TILE : k * TILE + size],
                    preferred_element_type=f32,
                )
                for k in range(width // TILE)
            ],
        )

    def add(parts, start=False):
        terms = [(features(place), ref, i) for place, ref, i in parts]
        for t in range(tiles):
            size = min(TILE, kept - t * TILE)
            y = functools.reduce(
                jnp.add, [turned_dot(x, ref, i, t, size) for x, ref, i in terms]
            )
            if start:
                acc[t, :, :size] = y
            else:
                acc[t, :, :size] += y

    def take(slot):
        wait_x(slot)
        x_copy(slot, x_rs.at[slot], f_ss, role, mate).start()

    def wait_far(i):
        place = relayed(i)
        wait_x(2 * place)
        wait_x(2 * place + 1)

    def take_direct(i):
        place = direct(i)
        take(2 * place)
        take(2 * place + 1)

    def near_term(i):
        return direct(i), turned, i

    def far_term(i):
        return relayed(i), near_head, i

    take(slot_of(1 - role, me))
    add([near_term(0)], True)
    turn(4)
    for i in range(1, SINGLE):
        take_direct(i)
        wait_far(i - 1)
        add([near_term(i), far_term(i - 1)])

    @pl.loop(SINGLE, chips)
    def _(i):
        take_direct(i)

    for i in range(SINGLE, chips, 2):
        for j in range(i, min(i + 2, chips)):
            wait_far(j - 1)
        parts = []
        for j in range(i, min(i + 2, chips)):
            parts += [near_term(j), far_term(j - 1)]
        if i + 2 >= chips:
            wait_far(chips - 1)
            parts.append(far_term(chips - 1))
        add(parts)

    landed(s_recv.at[pl.ds(0, 2 * n - 1)], s_rs)
    inverse = []
    for t in range(DECODE_STEPS):
        square = functools.reduce(jnp.add, [s_recv[(1 - t) * n + s] for s in range(n)])
        factor = lax.rsqrt(square / (n * width) + 1e-05)
        inverse.append(
            jnp.sum(jnp.where(diagonal == lane, factor, 0.0), axis=1, keepdims=True)
        )
    own_inverse = jnp.where(role == 0, inverse[1], inverse[0])
    inverse = jnp.concatenate(inverse, axis=0)
    action_rows = lax.broadcasted_iota(jnp.int32, (2 * rows, 1), 0)
    action = jnp.zeros((2 * rows, 1), jnp.int32)
    for t in range(DECODE_STEPS):
        for b in range(rows):
            action = jnp.where(action_rows == t * rows + b, actions[t, b], action)
    wanted = action - (me * vocab + first_row)
    twice = role * (2 * kept - vocab)
    tile_ids = lax.broadcasted_iota(jnp.int32, (2 * rows, TILE), 1)
    largest = jnp.full((2 * rows, 1), LOW, f32)
    logits = []
    for t in range(tiles):
        size = min(TILE, kept - t * TILE)
        tile = acc[t, :, :size] * inverse
        if t == 0:
            tile = jnp.where(tile_ids[:, :size] < twice, LOW, tile)
        logits.append(tile)
    whole = [tile for tile in logits if tile.shape[1] == TILE]
    largest = jnp.max(functools.reduce(jnp.maximum, whole), axis=1, keepdims=True)
    for tile in logits:
        if tile.shape[1] != TILE:
            largest = jnp.maximum(largest, jnp.max(tile, axis=1, keepdims=True))
    exp_sum = jnp.zeros((2 * rows, 1), f32)
    target = jnp.zeros((2 * rows, 1), f32)
    whole_sum = jnp.zeros((2 * rows, TILE), f32)
    whole_target = jnp.zeros((2 * rows, TILE), f32)
    for t, tile in enumerate(logits):
        size = tile.shape[1]
        here = tile_ids[:, :size] + t * TILE == wanted
        if t == 0:
            here = here & (tile_ids[:, :size] >= twice)
        power = jnp.exp(tile - largest)
        hit = jnp.where(here, tile, 0.0)
        if size == TILE:
            whole_sum += power
            whole_target += hit
        else:
            exp_sum += jnp.sum(power, axis=1, keepdims=True)
            target += jnp.sum(hit, axis=1, keepdims=True)
    exp_sum += jnp.sum(whole_sum, axis=1, keepdims=True)
    target += jnp.sum(whole_target, axis=1, keepdims=True)
    for t in range(DECODE_STEPS):
        part = slice(t * rows, (t + 1) * rows)
        packed = jnp.where(lane == diagonal, largest[part], 0.0)
        packed = jnp.where(lane == diagonal + rows, exp_sum[part], packed)
        packed = jnp.where(lane == diagonal + 2 * rows, target[part], packed)
        e_send[t] = jnp.sum(packed, axis=0, keepdims=True)
    for i in range(n - 1, -1, -1):
        to = flip(me, i, n)
        remote(e_send.at[1 - role], e_recv.at[own_stat], e_ss, e_rs, 1 - role, to).start()
        if i:
            remote(e_send.at[role], e_recv.at[own_stat], e_ss, e_rs, role, to).start()
    e_recv[own_stat] = e_send[role]

    n_send[...] = (state * own_inverse * gain[...]).astype(bf16)
    n_copy = remote(n_send, n_recv, n_sems.at[0], n_sems.at[1], 1 - role, me)
    n_copy.start()

    n_copy.wait_recv()
    normed[0] = n_recv[...]
    n_copy.wait_send()
    for i in range(1, chips):
        remote(q_own, q_all.at[own_slot], q_ss.at[i], q_rs.at[own_slot], role, me).wait_send()

    @pl.when(core != side)
    def _():
        remote(q_own, q_all.at[own_slot], q_ss.at[0], q_rs.at[own_slot], role, mate).wait_send()

    key_swap.wait_send()
    value_swap.wait_send()
    for i in range(near):
        for part in range(2):
            copy = remote(
                b_send.at[0], b_recv.at[chip], b_ss.at[2 * i + part], b_rs, role, me
            )
            if i == 0:

                @pl.when(core * half + 2 * (chip % near) + part != me)
                def _(copy=copy):
                    copy.wait_send()

            else:
                copy.wait_send()
    landed(c_send.at[pl.ds(0, n - 1)], c_ss)
    landed(x_all.at[pl.ds(0, n)], d_ss)
    landed(x_all.at[pl.ds(0, n - 1)], f_ss)
    landed(s_recv.at[pl.ds(0, 2 * n - 1)], s_ss)

    landed(e_recv.at[pl.ds(0, 2 * n - 1)], e_rs)
    got = [e_recv[s] for s in range(2 * n)]
    top = functools.reduce(jnp.maximum, got)
    exp_sum = jnp.zeros((1, HEAD_SIZE), f32)
    target = jnp.zeros((1, HEAD_SIZE), f32)
    stack = jnp.concatenate(got, axis=0)
    factor = pltpu.roll(jnp.exp(stack - top), rows, 1)
    exp_sum = jnp.sum(stack * factor, axis=0, keepdims=True)
    target = jnp.sum(stack, axis=0, keepdims=True)
    exp_sum = pltpu.roll(exp_sum, HEAD_SIZE - rows, 1)
    target = pltpu.roll(target, HEAD_SIZE - 2 * rows, 1)
    log_probs[...] = (target - top - jnp.log(exp_sum))[:, :rows]
    landed(e_recv.at[pl.ds(0, 2 * n - 1)], e_ss)


def hand_over(log_probs, normed, log_probs_out, normed_out, sems):
    copies = [
        pltpu.make_async_copy(log_probs, log_probs_out, sems.at[0]),
        pltpu.make_async_copy(normed, normed_out, sems.at[1]),
    ]
    for copy in copies:
        copy.start()
    for copy in copies:
        copy.wait()


def fused(
    queries,
    step_token_keys,
    step_token_values,
    stored_key_cache,
    stored_value_cache,
    lengths,
    wo_sides,
    gain_sides,
    head,
    resid,
    actions,
):
    tp = lax.axis_size("tp")
    n = lax.axis_size("grp") * tp
    rows = lengths.shape[0]
    width = resid.shape[2]
    heads = width // HEAD_SIZE
    kept = -(-head.shape[1] // 16) * 8
    tiles = -(-kept // TILE)
    shard = stored_key_cache.shape[1]
    slots = 2 * rows * shard
    half_keys = stored_key_cache.shape[2] // 2
    bf16, f32 = jnp.bfloat16, jnp.float32
    vmem = pl.BlockSpec(memory_space=pltpu.VMEM)
    hbm = pl.BlockSpec(memory_space=pl.ANY)
    message = heads * rows + rows
    dma = pltpu.SemaphoreType.DMA
    parts = pl.pallas_call(
        functools.partial(fused_kernel, n, tp),
        out_shape=(pltpu.VMEM((1, rows), f32), pltpu.VMEM((1, rows, width), bf16)),
        in_specs=[hbm] * 11,
        out_specs=(vmem, vmem),
        scratch_shapes=[
            pltpu.VMEM((rows, width), bf16),
            pltpu.VMEM((DECODE_STEPS, rows, HEAD_SIZE), bf16),
            pltpu.VMEM((DECODE_STEPS, rows, HEAD_SIZE), bf16),
            pltpu.SMEM((rows,), jnp.int32),
            pltpu.SMEM((DECODE_STEPS, rows), jnp.int32),
            pltpu.VMEM((1, width), f32),
            pltpu.VMEM((rows, width), bf16),
            pltpu.VMEM((2, rows, shard, half_keys), bf16),
            pltpu.VMEM((2, rows, shard, half_keys), bf16),
            pltpu.VMEM(wo_sides.shape[1:], bf16),
            pltpu.VMEM((n // 2, tiles * TILE, width), bf16),
            pltpu.VMEM((n // 2, tiles * TILE, width), bf16),
            pltpu.VMEM((n // 2, tiles * TILE, width), bf16),
            pltpu.VMEM((rows, slots), f32),
            pltpu.VMEM((n // 2, rows, width), bf16),
            pltpu.VMEM((n // 2, message, HEAD_SIZE), bf16),
            pltpu.VMEM((n // 2, message, HEAD_SIZE), bf16),
            pltpu.VMEM((n, rows, width), bf16),
            pltpu.VMEM((n, rows, width), bf16),
            pltpu.VMEM((2 * n, rows, width), bf16),
            pltpu.VMEM((1, HEAD_SIZE), f32),
            pltpu.VMEM((2 * n, 1, HEAD_SIZE), f32),
            pltpu.VMEM((tiles, 2 * rows, TILE), f32),
            pltpu.VMEM((rows, width), bf16),
            pltpu.VMEM((rows, width), bf16),
            pltpu.VMEM((2, 1, HEAD_SIZE), f32),
            pltpu.VMEM((2 * n, 1, HEAD_SIZE), f32),
            dma((10,)),
            dma((n,)),
            dma((n // 2,)),
            dma((n // 2,)),
            dma((2,)),
            dma((2,)),
            dma((n // 2,)),
            dma,
            dma,
            dma,
            dma,
            dma,
            dma((2 * n,)),
            dma,
            dma,
            dma((2,)),
            dma,
            dma,
        ],
        compiler_params=pltpu.CompilerParams(
            collective_id=0, has_side_effects=True, vmem_limit_bytes=60 * 1024 * 1024
        ),
    )(
        queries,
        step_token_keys,
        step_token_values,
        stored_key_cache,
        stored_value_cache,
        lengths,
        gain_sides,
        resid,
        actions,
        wo_sides,
        head.T,
    )
    return pl.pallas_call(
        hand_over,
        out_shape=tuple(jax.ShapeDtypeStruct(part.shape, part.dtype) for part in parts),
        in_specs=[vmem, vmem],
        out_specs=(hbm, hbm),
        scratch_shapes=[dma((2,))],
    )(*[pltpu.with_memory_space_constraint(part, pltpu.VMEM) for part in parts])


def on_device(*args):
    queries, lengths, head = args[0], args[5], args[8]
    tp = lax.axis_size("tp")
    n = lax.axis_size("grp") * tp
    width = queries.shape[2]
    group = QUERY_HEADS // KEY_VALUE_HEADS
    whole_heads = width % HEAD_SIZE == 0 and 2 * (width // HEAD_SIZE) == group
    powers = n & (n - 1) == 0 and n >= 8 and tp % 2 == 0 and n // 2 == KEY_VALUE_HEADS
    fits = lax.axis_size("role") == 2 and powers and lengths.shape[0] == 8
    if whole_heads and fits and head.shape[0] == n * width and head.shape[1] % 8 == 0:
        return fused(*args)
    return plain(*args)


def solution(mesh):
    in_specs = (
        P(None, None, ("grp", "tp")),
        P(),
        P(),
        P(None, ("grp", "tp"), None),
        P(None, ("grp", "tp"), None),
        P(),
        P("role", ("grp", "tp"), None),
        P("role", ("grp", "tp")),
        P(None, ("grp", "tp")),
        P(None, None, ("grp", "tp")),
        P(),
    )
    out_specs = (P("role", None), P("role", None, ("grp", "tp")))
    return jax.shard_map(
        on_device, mesh=mesh, in_specs=in_specs, out_specs=out_specs, check_vma=False
    )
```

```python
import functools
import math

import jax
import jax.numpy as jnp
from jax import lax
from jax.experimental import pallas as pl
from jax.experimental.pallas import tpu as pltpu
from jax.sharding import PartitionSpec as P

D = 8192
QUERY_HEADS = 64
KEY_VALUE_HEADS = 8
HEAD_SIZE = 128
DECODE_STEPS = 2


def swap_sides(value):
    return lax.ppermute(value, "role", [(0, 1), (1, 0)])


def plain(
    queries,
    step_token_keys,
    step_token_values,
    stored_key_cache,
    stored_value_cache,
    lengths,
    wo_sides,
    gain_sides,
    head,
    resid,
    actions,
):
    both = ("grp", "tp")
    place = lax.axis_index(both)
    step = 1 - lax.axis_index("role")
    count_of_rows = lengths.shape[0]
    shard_length = stored_key_cache.shape[1]
    query_group_width = QUERY_HEADS // KEY_VALUE_HEADS
    logit_scale = 1.0 / math.sqrt(HEAD_SIZE)
    query_matrix = lax.all_gather(
        lax.dynamic_index_in_dim(queries, step, 0, keepdims=False), both, axis=1, tiled=True
    )
    positions = place * shard_length + jnp.arange(shard_length, dtype=jnp.int32)
    valid = positions[None, :] < lengths[:, None]
    masking = valid[:, None, None, :]
    cache_shape = (count_of_rows, shard_length, KEY_VALUE_HEADS, HEAD_SIZE)
    prior_keys = stored_key_cache.reshape(cache_shape)
    prior_values = stored_value_cache.reshape(cache_shape)
    step_shape = (DECODE_STEPS, count_of_rows, KEY_VALUE_HEADS, HEAD_SIZE)
    incoming_keys = step_token_keys.astype(jnp.float32).reshape(step_shape)
    incoming_values = step_token_values.astype(jnp.float32).reshape(step_shape)
    current_query = query_matrix.reshape(
        count_of_rows, KEY_VALUE_HEADS, query_group_width, HEAD_SIZE
    )
    scores = (
        jnp.einsum("rkgd,rskd->rkgs", current_query, prior_keys, preferred_element_type=jnp.float32)
        * logit_scale
    )
    scores = jnp.where(masking, scores, -1e30)
    fresh_live = jnp.arange(DECODE_STEPS, dtype=jnp.int32) <= step
    fresh_scores = (
        jnp.einsum("rkgd,trkd->rkgt", current_query.astype(jnp.float32), incoming_keys)
        * logit_scale
    )
    fresh_scores = jnp.where(fresh_live, fresh_scores, -1e30)
    fresh_highest = jnp.max(fresh_scores, axis=-1)
    overall = lax.pmax(jnp.maximum(jnp.max(scores, axis=-1), fresh_highest), both)
    cache_probs = jnp.exp(scores - overall[..., None]) * masking
    fresh_probs = jnp.exp(fresh_scores - overall[..., None]) * fresh_live
    fresh_probs = fresh_probs * (place == 0)
    totals = jnp.sum(cache_probs, axis=-1) + jnp.sum(fresh_probs, axis=-1)
    weighted = jnp.einsum(
        "rkgs,rskd->rkgd", cache_probs, prior_values.astype(jnp.float32)
    ) + jnp.einsum("rkgt,trkd->rkgd", fresh_probs, incoming_values)
    features = QUERY_HEADS * HEAD_SIZE
    mixed = lax.psum_scatter(
        weighted.reshape(count_of_rows, features), both, scatter_dimension=1, tiled=True
    )
    totals = lax.psum(totals.reshape(count_of_rows, QUERY_HEADS), both)
    feature_rows = wo_sides.shape[1]
    own_heads = (place * feature_rows + jnp.arange(feature_rows)) // HEAD_SIZE
    own_part = (mixed / jnp.take(totals, own_heads, axis=1)).astype(jnp.bfloat16)
    branch_out = lax.psum_scatter(
        jnp.dot(own_part, wo_sides[0], preferred_element_type=jnp.float32),
        both,
        scatter_dimension=1,
        tiled=True,
    )
    resid_now = lax.dynamic_index_in_dim(resid, step, 0, keepdims=False)
    state = resid_now.astype(jnp.float32) + branch_out
    square_sum = lax.psum(jnp.sum(state * state, axis=-1), both)
    normed_now = (
        state * lax.rsqrt(square_sum[:, None] / D + 1e-05) * gain_sides[0][None, :]
    ).astype(jnp.bfloat16)
    logits = jnp.dot(
        lax.all_gather(normed_now, both, axis=1, tiled=True),
        head,
        preferred_element_type=jnp.float32,
    )
    local_highest = jnp.max(logits, axis=-1)
    action_now = lax.dynamic_index_in_dim(actions, step, 0, keepdims=False)
    head_width = head.shape[1]
    vocab_ids = place * head_width + jnp.arange(head_width, dtype=jnp.int32)
    is_target = vocab_ids[None, :] == action_now[:, None]
    target = jnp.sum(jnp.where(is_target, logits, 0.0), axis=-1)
    exp_sum = jnp.sum(jnp.exp(logits - local_highest[:, None]), axis=-1)
    parts = lax.all_gather(jnp.stack([local_highest, exp_sum, target]), both)
    largest = jnp.max(parts[:, 0], axis=0)
    exp_sum = jnp.sum(parts[:, 1] * jnp.exp(parts[:, 0] - largest[None]), axis=0)
    prob_now = jnp.sum(parts[:, 2], axis=0) - largest - jnp.log(exp_sum)
    return (swap_sides(prob_now)[None], swap_sides(normed_now)[None])


LOW = -1e30
DEAD = -1e29
TILE = 256
SINGLE = 3
FIRST = 4
TURNS = (4, 3, 5, 3, 1)
MESH = pl.DeviceIdType.MESH


def fused_kernel(
    n,
    tp,
    queries,
    token_keys,
    token_values,
    keys_in,
    values_in,
    lengths_in,
    gain_in,
    resid_in,
    actions_in,
    wo,
    head,
    log_probs,
    normed,
    q_own,
    fresh_keys,
    fresh_values,
    lengths,
    actions,
    gain,
    resid,
    keys,
    values,
    wo_buf,
    near_head,
    far_head,
    turned,
    bias,
    q_all,
    b_send,
    b_recv,
    c_send,
    c_recv,
    x_all,
    s_send,
    s_recv,
    acc,
    n_send,
    n_recv,
    e_send,
    e_recv,
    in_sems,
    head_sems,
    q_ss,
    q_rs,
    k_ss,
    k_rs,
    b_ss,
    b_rs,
    c_ss,
    c_rs,
    d_ss,
    f_ss,
    x_rs,
    s_ss,
    s_rs,
    n_sems,
    e_ss,
    e_rs,
):
    role = lax.axis_index("role")
    grp = lax.axis_index("grp")
    lane_of = lax.axis_index("tp")
    me = grp * tp + lane_of
    core = me % 2
    chip = me // 2
    mate = me + 1 - 2 * core
    chips = n // 2
    near = chips // 2
    half = n // 2
    side = grp
    step = 1 - role
    rows = resid.shape[0]
    width = resid.shape[1]
    shard = keys.shape[2]
    half_keys = keys.shape[3]
    own_heads = width // HEAD_SIZE
    group = QUERY_HEADS // KEY_VALUE_HEADS
    slots = 2 * rows * shard
    vocab = head.shape[0]
    kept = -(-vocab // 16) * 8
    tiles = acc.shape[0]
    scale = 1.0 / math.sqrt(HEAD_SIZE)
    f32 = jnp.float32
    bf16 = jnp.bfloat16

    def flip(index, by, size):
        out = index
        bit = 1
        while bit < size:
            if isinstance(by, int):
                if by // bit % 2:
                    out = out + bit - 2 * bit * (index // bit % 2)
            else:
                out = out + (by // bit % 2) * (bit - 2 * bit * (index // bit % 2))
            bit *= 2
        return out

    steps_of = [lane_of]
    bit = 1
    while bit < tp:
        change = bit - 2 * bit * (lane_of // bit % 2)
        steps_of += [at + change for at in steps_of]
        bit *= 2
    grps = (grp, 1 - grp)
    roles = (role, 1 - role)

    def peer(i, other_role=0):
        return roles[other_role], grps[i // tp], steps_of[i % tp]

    def remote(src, dst, ss, rs, where):
        return pltpu.make_async_remote_copy(
            src_ref=src,
            dst_ref=dst,
            send_sem=ss,
            recv_sem=rs,
            device_id=where,
            device_id_type=MESH,
        )

    here = peer(0)
    mate_at = peer(1)

    def landed(ref, sem):
        pltpu.make_async_copy(ref, ref, sem).wait()

    own_keys = pl.ds(pl.multiple_of(core * half_keys, 128), half_keys)
    mate_keys = pl.ds(pl.multiple_of((1 - core) * half_keys, 128), half_keys)
    chip_lanes = pl.ds(pl.multiple_of(chip * HEAD_SIZE, HEAD_SIZE), HEAD_SIZE)
    loads = [
        pltpu.make_async_copy(src, dst, in_sems.at[i])
        for i, (src, dst) in enumerate(
            [
                (queries.at[step], q_own),
                (lengths_in, lengths),
                (keys_in.at[:, :, own_keys], keys.at[core]),
                (values_in.at[:, :, own_keys], values.at[core]),
                (token_keys.at[:, :, chip_lanes], fresh_keys),
                (token_values.at[:, :, chip_lanes], fresh_values),
                (resid_in.at[step], resid),
                (gain_in, gain),
                (actions_in, actions),
                (wo.at[0], wo_buf),
            ]
        )
    ]
    loads[0].start()
    barrier = pltpu.get_barrier_semaphore()
    for i in range(1, 2 * n):
        pl.semaphore_signal(
            barrier, inc=1, device_id=peer(i % n, i // n), device_id_type=MESH
        )
    first_row = pl.multiple_of(role * (vocab - kept), 8)

    def direct(i):
        return 2 * flip(chip, i, chips) + core

    def relayed(i):
        return 2 * flip(chip, i, chips) + 1 - core

    def head_copy(place, buf, i, sem):
        lanes = pl.ds(pl.multiple_of(place * width, 128), width)
        return pltpu.make_async_copy(
            head.at[pl.ds(first_row, kept), lanes], buf.at[i, pl.ds(0, kept), :], head_sems.at[sem]
        )

    def near_copy(i):
        return head_copy(direct(i), near_head, i, i)

    def far_copy(i):
        return head_copy(relayed(i), far_head, i, chips + i)

    for copy in loads[1:-1]:
        copy.start()
    for i in range(FIRST):
        near_copy(i).start()
    loads[-1].start()
    for i in range(FIRST, chips):
        near_copy(i).start()
    pl.semaphore_wait(barrier, 2 * n - 1)
    loads[0].wait()

    own_slot = me % half
    for i in range(chips - 1, 0, -1):
        _, to_grp, to_lane = peer(2 * i)
        to = role, to_grp, to_lane - core + side
        remote(q_own, q_all.at[own_slot], q_ss.at[i], q_rs.at[own_slot], to).start()

    @pl.when(core != side)
    def _():
        remote(q_own, q_all.at[own_slot], q_ss.at[0], q_rs.at[own_slot], mate_at).start()

    @pl.when(core == side)
    def _():
        q_all[own_slot] = q_own[...]

    key_swap = remote(
        keys_in.at[:, :, mate_keys], keys.at[core], k_ss.at[0], k_rs.at[0], mate_at
    )
    value_swap = remote(
        values_in.at[:, :, mate_keys], values.at[core], k_ss.at[1], k_rs.at[1], mate_at
    )
    key_swap.start()
    value_swap.start()

    loads[1].wait()
    row_ids = lax.broadcasted_iota(jnp.int32, (rows, slots), 0)
    col_ids = lax.broadcasted_iota(jnp.int32, (rows, slots), 1)
    limit = jnp.zeros((rows, slots), jnp.int32)
    for b in range(rows):
        limit = jnp.where(row_ids == b, lengths[b], limit)
    origin = col_ids // (rows * shard)
    place_ids = (2 * chip + origin) * shard + col_ids % shard
    live = (col_ids // shard % rows == row_ids) & (place_ids < limit)
    bias[...] = jnp.where(live, 0.0, LOW)

    def turn_one(copy, source, target, i, j):
        copy(i).wait()
        for t in range(tiles):
            size = min(TILE, kept - t * TILE)
            tile = source[i, t * TILE : t * TILE + size, :].T
            for k in range(width // TILE):
                target[j, t * TILE : (t + 1) * TILE, k * TILE : k * TILE + size] = tile[
                    k * TILE : (k + 1) * TILE
                ]

    def turn(window):
        first = sum(TURNS[:window])
        last = first + TURNS[window]

        @pl.loop(min(first, chips), min(last, chips))
        def _(i):
            turn_one(near_copy, near_head, turned, i, i)

        @pl.loop(max(first - chips, 0), max(last - chips, 0))
        def _(i):
            turn_one(far_copy, far_head, near_head, i, i)

    turn(0)
    loads[2].wait()
    loads[3].wait()
    ones = jnp.ones((slots, HEAD_SIZE), bf16)
    lane = lax.broadcasted_iota(jnp.int32, (rows, HEAD_SIZE), 1)

    def wait_query(slot):
        remote(q_own, q_all.at[slot], q_ss.at[0], q_rs.at[slot], here).wait_recv()

    for i in range(near):
        local = flip(chip % near, i, near)
        slot = 2 * local
        if i == 0:

            @pl.when(core == side)
            def _():
                wait_query(mate % half)

            @pl.when(core != side)
            def _():
                wait_query(slot)
                wait_query(slot + 1)

            remote(
                keys_in.at[:, :, mate_keys], keys.at[1 - core], k_ss.at[0], k_rs.at[0], here
            ).wait_recv()
            remote(
                values_in.at[:, :, mate_keys], values.at[1 - core], k_ss.at[1], k_rs.at[1], here
            ).wait_recv()
        else:
            wait_query(slot)
            wait_query(slot + 1)
        lanes = pl.ds(pl.multiple_of(local * HEAD_SIZE, HEAD_SIZE), HEAD_SIZE)
        query = jnp.concatenate(
            [
                q_all[slot + part, :, j * HEAD_SIZE : (j + 1) * HEAD_SIZE].astype(f32)
                for part in range(2)
                for j in range(own_heads)
            ],
            axis=0,
        ).astype(bf16)
        key = keys[:, :, :, lanes].reshape(slots, HEAD_SIZE)
        value = values[:, :, :, lanes].reshape(slots, HEAD_SIZE)
        scores = lax.dot_general(query, key, (((1,), (1,)), ((), ())), preferred_element_type=f32)
        scores = (scores * scale).reshape(group, rows, slots) + bias[...][None]
        scores = scores.reshape(group * rows, slots)
        top = jnp.max(scores, axis=1, keepdims=True)
        top = jnp.maximum(top, DEAD).astype(bf16).astype(f32)
        probs = jnp.exp(scores - top).astype(bf16)
        both = jnp.dot(
            probs, jnp.concatenate([value, ones], axis=1), preferred_element_type=f32
        )
        weighted = both[:, :HEAD_SIZE]
        total = both[:, HEAD_SIZE:]
        total_high = total.astype(bf16).astype(f32)
        total_low = total - total_high
        for part in range(2):
            stats = jnp.zeros((rows, HEAD_SIZE), f32)
            for j in range(own_heads):
                at = (part * own_heads + j) * rows
                stats = jnp.where(lane == j, top[at : at + rows], stats)
                stats = jnp.where(lane == own_heads + j, total_high[at : at + rows], stats)
                stats = jnp.where(lane == 2 * own_heads + j, total_low[at : at + rows], stats)
            first = part * own_heads * rows
            b_send[slot + part] = jnp.concatenate(
                [weighted[first : first + own_heads * rows], stats], axis=0
            ).astype(bf16)
        for part in range(2):
            to = core * half + slot + part
            where = role, core, steps_of[2 * i] - core + part
            copy = remote(
                b_send.at[slot + part], b_recv.at[chip], b_ss.at[2 * i + part], b_rs, where
            )
            if i == 0:

                @pl.when(to != me)
                def _(copy=copy):
                    copy.start()

                @pl.when(to == me)
                def _(part=part):
                    b_recv[chip] = b_send[slot + part]

            else:
                copy.start()

    for i in range(chips):
        far_copy(i).start()
    for copy in loads[4:9]:
        copy.wait()
    own_query = q_own[...].astype(f32)
    fresh = []
    for u in range(DECODE_STEPS):
        fresh_key = fresh_keys[u].astype(f32)
        fresh.append(
            [
                jnp.where(
                    u <= step,
                    jnp.sum(
                        own_query[:, j * HEAD_SIZE : (j + 1) * HEAD_SIZE] * fresh_key,
                        axis=1,
                        keepdims=True,
                    )
                    * scale,
                    LOW,
                )
                for j in range(own_heads)
            ]
        )

    turn(1)

    @pl.when(core == side)
    def _():
        landed(b_recv.at[pl.ds(0, chips - 1)], b_rs)

    @pl.when(core != side)
    def _():
        landed(b_recv, b_rs)

    stats = [b_recv[s, own_heads * rows :, :].astype(f32) for s in range(chips)]
    top = functools.reduce(jnp.maximum, stats)
    tops = [
        functools.reduce(
            jnp.maximum, [fresh[u][j] for u in range(DECODE_STEPS)], top[:, j : j + 1]
        )
        for j in range(own_heads)
    ]
    numerator = [jnp.zeros((rows, HEAD_SIZE), f32) for _ in range(own_heads)]
    denominator = [jnp.zeros((rows, 1), f32) for _ in range(own_heads)]
    for j in range(own_heads):
        for u in range(DECODE_STEPS):
            weight = jnp.where(u <= step, jnp.exp(fresh[u][j] - tops[j]), 0.0)
            numerator[j] += weight * fresh_values[u].astype(f32)
            denominator[j] += weight
    for s in range(chips):
        part = b_recv[s, : own_heads * rows, :].astype(f32)
        for j in range(own_heads):
            factor = jnp.exp(stats[s][:, j : j + 1] - tops[j])
            numerator[j] += factor * part[j * rows : (j + 1) * rows]
            at = own_heads + j
            denominator[j] += factor * (
                stats[s][:, at : at + 1] + stats[s][:, at + own_heads : at + own_heads + 1]
            )
    attended = jnp.concatenate(
        [numerator[j] / denominator[j] for j in range(own_heads)], axis=1
    ).astype(bf16)

    loads[9].wait()
    block = 4
    for i in range(n // block - 1, -1, -1):
        base = flip(me // block, i, n // block) * block
        out = jnp.dot(
            attended,
            wo_buf[:, pl.ds(pl.multiple_of(base * width, 128), block * width)],
            preferred_element_type=f32,
        )
        for j in range(block):
            c_send[base + j] = out[:, j * width : (j + 1) * width].astype(bf16)
        for j in range(block):
            to = base + j
            _, to_grp, to_lane = peer(block * i)
            where = role, to_grp, to_lane - me % block + j
            copy = remote(c_send.at[to], c_recv.at[me], c_ss, c_rs, where)
            if i == 0:

                @pl.when(to != me)
                def _(copy=copy):
                    copy.start()

            else:
                copy.start()
    state = resid[...].astype(f32)
    c_recv[me] = c_send[me]

    turn(2)
    landed(c_recv.at[pl.ds(0, n - 1)], c_rs)
    for s in range(n):
        state += c_recv[s].astype(f32)

    def slot_of(from_role, place):
        return 2 * place + 1 - from_role

    mine = slot_of(role, me)
    x_all[mine] = (state * gain[...]).astype(bf16)

    def x_copy(slot, rs, ss, where):
        return remote(x_all.at[slot], x_all.at[slot], ss, rs, where)

    for i in range(chips):
        x_copy(mine, x_rs.at[mine], d_ss, peer(2 * i, 1)).start()
        x_copy(mine, x_rs.at[mine], d_ss, peer(2 * i) if i else mate_at).start()

    diagonal = lax.broadcasted_iota(jnp.int32, (rows, HEAD_SIZE), 0)
    square = jnp.sum(state * state, axis=1, keepdims=True)
    s_send[...] = jnp.sum(jnp.where(diagonal == lane, square, 0.0), axis=0, keepdims=True)
    own_stat = role * n + me
    for i in range(n - 1, -1, -1):
        remote(s_send, s_recv.at[own_stat], s_ss, s_rs, peer(i, 1)).start()
        if i:
            remote(s_send, s_recv.at[own_stat], s_ss, s_rs, peer(i)).start()
    s_recv[own_stat] = s_send[...]

    turn(3)

    def wait_x(slot):
        x_copy(slot, x_rs.at[slot], d_ss, here).wait_recv()

    def features(place):
        return jnp.concatenate(
            [x_all[2 * place].astype(f32), x_all[2 * place + 1].astype(f32)], axis=0
        ).astype(bf16)

    def turned_dot(x, ref, i, t, size):
        return functools.reduce(
            jnp.add,
            [
                jnp.dot(
                    x[:, k * TILE : (k + 1) * TILE],
                    ref[i, t * TILE : (t + 1) * TILE, k * TILE : k * TILE + size],
                    preferred_element_type=f32,
                )
                for k in range(width // TILE)
            ],
        )

    def add(parts, start=False):
        terms = [(features(place), ref, i) for place, ref, i in parts]
        for t in range(tiles):
            size = min(TILE, kept - t * TILE)
            y = functools.reduce(
                jnp.add, [turned_dot(x, ref, i, t, size) for x, ref, i in terms]
            )
            if start:
                acc[t, :, :size] = y
            else:
                acc[t, :, :size] += y

    def take(slot):
        wait_x(slot)
        x_copy(slot, x_rs.at[slot], f_ss, mate_at).start()

    def wait_far(i):
        place = relayed(i)
        wait_x(2 * place)
        wait_x(2 * place + 1)

    def take_direct(i):
        place = direct(i)
        take(2 * place)
        take(2 * place + 1)

    def near_term(i):
        return direct(i), turned, i

    def far_term(i):
        return relayed(i), near_head, i

    take(slot_of(1 - role, me))
    add([near_term(0)], True)
    turn(4)
    for i in range(1, SINGLE):
        take_direct(i)
        wait_far(i - 1)
        add([near_term(i), far_term(i - 1)])

    @pl.loop(SINGLE, chips)
    def _(i):
        take_direct(i)

    for i in range(SINGLE, chips, 2):
        for j in range(i, min(i + 2, chips)):
            wait_far(j - 1)
        parts = []
        for j in range(i, min(i + 2, chips)):
            parts += [near_term(j), far_term(j - 1)]
        if i + 2 >= chips:
            wait_far(chips - 1)
            parts.append(far_term(chips - 1))
        add(parts)

    landed(s_recv.at[pl.ds(0, 2 * n - 1)], s_rs)
    inverse = []
    for t in range(DECODE_STEPS):
        square = functools.reduce(jnp.add, [s_recv[(1 - t) * n + s] for s in range(n)])
        factor = lax.rsqrt(square / (n * width) + 1e-05)
        inverse.append(
            jnp.sum(jnp.where(diagonal == lane, factor, 0.0), axis=1, keepdims=True)
        )
    own_inverse = jnp.where(role == 0, inverse[1], inverse[0])
    inverse = jnp.concatenate(inverse, axis=0)
    action_rows = lax.broadcasted_iota(jnp.int32, (2 * rows, 1), 0)
    action = jnp.zeros((2 * rows, 1), jnp.int32)
    for t in range(DECODE_STEPS):
        for b in range(rows):
            action = jnp.where(action_rows == t * rows + b, actions[t, b], action)
    wanted = action - (me * vocab + first_row)
    twice = role * (2 * kept - vocab)
    tile_ids = lax.broadcasted_iota(jnp.int32, (2 * rows, TILE), 1)
    largest = jnp.full((2 * rows, 1), LOW, f32)
    logits = []
    for t in range(tiles):
        size = min(TILE, kept - t * TILE)
        tile = acc[t, :, :size] * inverse
        if t == 0:
            tile = jnp.where(tile_ids[:, :size] < twice, LOW, tile)
        logits.append(tile)
    whole = [tile for tile in logits if tile.shape[1] == TILE]
    largest = jnp.max(functools.reduce(jnp.maximum, whole), axis=1, keepdims=True)
    for tile in logits:
        if tile.shape[1] != TILE:
            largest = jnp.maximum(largest, jnp.max(tile, axis=1, keepdims=True))
    exp_sum = jnp.zeros((2 * rows, 1), f32)
    target = jnp.zeros((2 * rows, 1), f32)
    whole_sum = jnp.zeros((2 * rows, TILE), f32)
    whole_target = jnp.zeros((2 * rows, TILE), f32)
    for t, tile in enumerate(logits):
        size = tile.shape[1]
        here = tile_ids[:, :size] + t * TILE == wanted
        if t == 0:
            here = here & (tile_ids[:, :size] >= twice)
        power = jnp.exp(tile - largest)
        hit = jnp.where(here, tile, 0.0)
        if size == TILE:
            whole_sum += power
            whole_target += hit
        else:
            exp_sum += jnp.sum(power, axis=1, keepdims=True)
            target += jnp.sum(hit, axis=1, keepdims=True)
    exp_sum += jnp.sum(whole_sum, axis=1, keepdims=True)
    target += jnp.sum(whole_target, axis=1, keepdims=True)
    for t in range(DECODE_STEPS):
        part = slice(t * rows, (t + 1) * rows)
        packed = jnp.where(lane == diagonal, largest[part], 0.0)
        packed = jnp.where(lane == diagonal + rows, exp_sum[part], packed)
        packed = jnp.where(lane == diagonal + 2 * rows, target[part], packed)
        e_send[t] = jnp.sum(packed, axis=0, keepdims=True)
    for i in range(n - 1, -1, -1):
        remote(e_send.at[1 - role], e_recv.at[own_stat], e_ss, e_rs, peer(i, 1)).start()
        if i:
            remote(e_send.at[role], e_recv.at[own_stat], e_ss, e_rs, peer(i)).start()
    e_recv[own_stat] = e_send[role]

    n_send[...] = (state * own_inverse * gain[...]).astype(bf16)
    n_copy = remote(n_send, n_recv, n_sems.at[0], n_sems.at[1], peer(0, 1))
    n_copy.start()

    n_copy.wait_recv()
    normed[0] = n_recv[...]
    n_copy.wait_send()
    for i in range(1, chips):
        remote(q_own, q_all.at[own_slot], q_ss.at[i], q_rs.at[own_slot], here).wait_send()

    @pl.when(core != side)
    def _():
        remote(q_own, q_all.at[own_slot], q_ss.at[0], q_rs.at[own_slot], mate_at).wait_send()

    key_swap.wait_send()
    value_swap.wait_send()
    for i in range(near):
        for part in range(2):
            copy = remote(
                b_send.at[0], b_recv.at[chip], b_ss.at[2 * i + part], b_rs, here
            )
            if i == 0:

                @pl.when(core * half + 2 * (chip % near) + part != me)
                def _(copy=copy):
                    copy.wait_send()

            else:
                copy.wait_send()
    landed(c_send.at[pl.ds(0, n - 1)], c_ss)
    landed(x_all.at[pl.ds(0, n)], d_ss)
    landed(x_all.at[pl.ds(0, n - 1)], f_ss)
    landed(s_recv.at[pl.ds(0, 2 * n - 1)], s_ss)

    landed(e_recv.at[pl.ds(0, 2 * n - 1)], e_rs)
    got = [e_recv[s] for s in range(2 * n)]
    top = functools.reduce(jnp.maximum, got)
    exp_sum = jnp.zeros((1, HEAD_SIZE), f32)
    target = jnp.zeros((1, HEAD_SIZE), f32)
    stack = jnp.concatenate(got, axis=0)
    factor = pltpu.roll(jnp.exp(stack - top), rows, 1)
    exp_sum = jnp.sum(stack * factor, axis=0, keepdims=True)
    target = jnp.sum(stack, axis=0, keepdims=True)
    exp_sum = pltpu.roll(exp_sum, HEAD_SIZE - rows, 1)
    target = pltpu.roll(target, HEAD_SIZE - 2 * rows, 1)
    log_probs[...] = (target - top - jnp.log(exp_sum))[:, :rows]
    landed(e_recv.at[pl.ds(0, 2 * n - 1)], e_ss)


def hand_over(log_probs, normed, log_probs_out, normed_out, sems):
    copies = [
        pltpu.make_async_copy(log_probs, log_probs_out, sems.at[0]),
        pltpu.make_async_copy(normed, normed_out, sems.at[1]),
    ]
    for copy in copies:
        copy.start()
    for copy in copies:
        copy.wait()


def fused(
    queries,
    step_token_keys,
    step_token_values,
    stored_key_cache,
    stored_value_cache,
    lengths,
    wo_sides,
    gain_sides,
    head,
    resid,
    actions,
):
    tp = lax.axis_size("tp")
    n = lax.axis_size("grp") * tp
    rows = lengths.shape[0]
    width = resid.shape[2]
    heads = width // HEAD_SIZE
    kept = -(-head.shape[1] // 16) * 8
    tiles = -(-kept // TILE)
    shard = stored_key_cache.shape[1]
    slots = 2 * rows * shard
    half_keys = stored_key_cache.shape[2] // 2
    bf16, f32 = jnp.bfloat16, jnp.float32
    vmem = pl.BlockSpec(memory_space=pltpu.VMEM)
    hbm = pl.BlockSpec(memory_space=pl.ANY)
    message = heads * rows + rows
    dma = pltpu.SemaphoreType.DMA
    parts = pl.pallas_call(
        functools.partial(fused_kernel, n, tp),
        out_shape=(pltpu.VMEM((1, rows), f32), pltpu.VMEM((1, rows, width), bf16)),
        in_specs=[hbm] * 11,
        out_specs=(vmem, vmem),
        scratch_shapes=[
            pltpu.VMEM((rows, width), bf16),
            pltpu.VMEM((DECODE_STEPS, rows, HEAD_SIZE), bf16),
            pltpu.VMEM((DECODE_STEPS, rows, HEAD_SIZE), bf16),
            pltpu.SMEM((rows,), jnp.int32),
            pltpu.SMEM((DECODE_STEPS, rows), jnp.int32),
            pltpu.VMEM((1, width), f32),
            pltpu.VMEM((rows, width), bf16),
            pltpu.VMEM((2, rows, shard, half_keys), bf16),
            pltpu.VMEM((2, rows, shard, half_keys), bf16),
            pltpu.VMEM(wo_sides.shape[1:], bf16),
            pltpu.VMEM((n // 2, tiles * TILE, width), bf16),
            pltpu.VMEM((n // 2, tiles * TILE, width), bf16),
            pltpu.VMEM((n // 2, tiles * TILE, width), bf16),
            pltpu.VMEM((rows, slots), f32),
            pltpu.VMEM((n // 2, rows, width), bf16),
            pltpu.VMEM((n // 2, message, HEAD_SIZE), bf16),
            pltpu.VMEM((n // 2, message, HEAD_SIZE), bf16),
            pltpu.VMEM((n, rows, width), bf16),
            pltpu.VMEM((n, rows, width), bf16),
            pltpu.VMEM((2 * n, rows, width), bf16),
            pltpu.VMEM((1, HEAD_SIZE), f32),
            pltpu.VMEM((2 * n, 1, HEAD_SIZE), f32),
            pltpu.VMEM((tiles, 2 * rows, TILE), f32),
            pltpu.VMEM((rows, width), bf16),
            pltpu.VMEM((rows, width), bf16),
            pltpu.VMEM((2, 1, HEAD_SIZE), f32),
            pltpu.VMEM((2 * n, 1, HEAD_SIZE), f32),
            dma((10,)),
            dma((n,)),
            dma((n // 2,)),
            dma((n // 2,)),
            dma((2,)),
            dma((2,)),
            dma((n // 2,)),
            dma,
            dma,
            dma,
            dma,
            dma,
            dma((2 * n,)),
            dma,
            dma,
            dma((2,)),
            dma,
            dma,
        ],
        compiler_params=pltpu.CompilerParams(
            collective_id=0, has_side_effects=True, vmem_limit_bytes=60 * 1024 * 1024
        ),
    )(
        queries,
        step_token_keys,
        step_token_values,
        stored_key_cache,
        stored_value_cache,
        lengths,
        gain_sides,
        resid,
        actions,
        wo_sides,
        head.T,
    )
    return pl.pallas_call(
        hand_over,
        out_shape=tuple(jax.ShapeDtypeStruct(part.shape, part.dtype) for part in parts),
        in_specs=[vmem, vmem],
        out_specs=(hbm, hbm),
        scratch_shapes=[dma((2,))],
    )(*[pltpu.with_memory_space_constraint(part, pltpu.VMEM) for part in parts])


def on_device(*args):
    queries, lengths, head = args[0], args[5], args[8]
    tp = lax.axis_size("tp")
    n = lax.axis_size("grp") * tp
    width = queries.shape[2]
    group = QUERY_HEADS // KEY_VALUE_HEADS
    whole_heads = width % HEAD_SIZE == 0 and 2 * (width // HEAD_SIZE) == group
    powers = n & (n - 1) == 0 and n >= 8 and tp % 2 == 0 and n // 2 == KEY_VALUE_HEADS == tp
    fits = lax.axis_size("role") == 2 and powers and lengths.shape[0] == 8
    if whole_heads and fits and head.shape[0] == n * width and head.shape[1] % 8 == 0:
        return fused(*args)
    return plain(*args)


def solution(mesh):
    in_specs = (
        P(None, None, ("grp", "tp")),
        P(),
        P(),
        P(None, ("grp", "tp"), None),
        P(None, ("grp", "tp"), None),
        P(),
        P("role", ("grp", "tp"), None),
        P("role", ("grp", "tp")),
        P(None, ("grp", "tp")),
        P(None, None, ("grp", "tp")),
        P(),
    )
    out_specs = (P("role", None), P("role", None, ("grp", "tp")))
    return jax.shard_map(
        on_device, mesh=mesh, in_specs=in_specs, out_specs=out_specs, check_vma=False
    )
```
